128 devices in a mesh: rep: 16 (over x, y_lo, core), tp: 8 (over z, y_hi).
Axes of the slice: x: 4, y: 4 (y_hi: 2, y_lo: 2; y = y_hi * 2 + y_lo), z: 4, core: 2. Of those that a mesh axis runs over, the one named last changes fastest.
Arguments:
- context: bfloat16 [32768, 5120], P('rep', 'tp'), may hold values from -6 to 6
- out_grad: bfloat16 [32768, 5120], P('rep', 'tp'), may hold values from -6 to 6
- rewards: int32 [8, 64], P(None, 'rep'), may hold values from 0 to 1
- master: float32 [5120, 5120], P('rep', 'tp'), may hold values from -0.078125 to 0.078125
- first_moment: float32 [5120, 5120], P('rep', 'tp'), may hold values from -0.03125 to 0.03125
- second_moment: float32 [5120, 5120], P('rep', 'tp'), may hold values from 3.0517577e-07 to 3.0517578e-05
- inputs: bfloat16 [4, 512, 5120], P(None, 'rep'), may hold values from -6 to 6
- w_query: bfloat16 [5120, 5120], P(None, 'tp'), may hold values from -0.078125 to 0.078125
- w_key: bfloat16 [5120, 1024], P(None, 'tp'), may hold values from -0.078125 to 0.078125
- w_value: bfloat16 [5120, 1024], P(None, 'tp'), may hold values from -0.078125 to 0.078125
- cache_keys: bfloat16 [512, 256, 1024], P('rep', None, 'tp'), may hold values from -400 to 400
- cache_values: bfloat16 [512, 256, 1024], P('rep', None, 'tp'), may hold values from -24 to 24
- lengths: int32 [64], P('rep'), may hold values from 64 to 256
Outputs:
- decoded: bfloat16 [4, 512, 5120], P(None, 'rep')
- adam_step: float32 [5120, 5120], P('rep', 'tp')
The draws below stay inside these ranges and needn't reach their ends.
All inputs are finite; a program needn't handle non-finite values.
Results may differ from the reference program's by a relative error of at most 0.0088.
Values may be sent and summed in bfloat16 or wider, within the bound.
A program may use at most 128 MiB of HBM per device.

```python
import math
import jax
import jax.numpy as jnp
from jax import lax

D = 5120
HEADS = 40
KV_HEADS = 8
HEAD_DIM = 128
PROMPTS_L = 8
GROUP_DEV = 4
RESP_LEN = 64
CACHE = 256
ROLL_SAMP = 8
STEPS = 4
GROUP = 64
TOK_DEV = 2048
TOKENS = 32768
SEQS = 512
RPROMPTS = 64
N_REP = 16


def draw_rewards(key, part):
    sample_index = jnp.arange(GROUP, dtype=jnp.int32)[None, :]
    threshold = 150 + 700 * sample_index // (GROUP - 1)
    ticket = jax.random.randint(jax.random.fold_in(key, 21), (PROMPTS_L, GROUP), 0, 1000)
    return (ticket < threshold).astype(jnp.int32)


def draw_cache_keys(key, part):
    base = jax.random.normal(jax.random.fold_in(key, 11), (SEQS, CACHE, KV_HEADS * HEAD_DIM), jnp.float32)
    base = jnp.clip(base, -6.0, 6.0)
    return base.astype(jnp.bfloat16)


def set_ends(array, key, smallest, largest):
    longest = array.shape.index(max(array.shape))
    spots = []
    for shift in (0, 1):
        where = [jax.random.randint(jax.random.fold_in(key, axis), (), 0, length) for axis, length in enumerate(array.shape)]
        where[longest] = (where[longest] + shift) % array.shape[longest]
        spots.append(tuple(where))
    return array.at[spots[0]].set(smallest).at[spots[1]].set(largest)


def with_spikes(drawn, stream_key, source, target, shards_of, factor):
    def block_of(dim):
        return (jnp.arange(drawn.shape[dim]) // (drawn.shape[dim] // shards_of)).reshape((-1,) + (1,) * (drawn.ndim - 1 - dim))

    near = jax.random.permutation(stream_key, shards_of)[block_of(target)]
    far = (block_of(target) + shards_of // 2) % shards_of
    return jnp.where((block_of(source) == near) | (block_of(source) == far), factor * drawn, drawn)


def levels(key, dims, shards, least, top_value):
    factor_of = 1.0
    for position, shards_of in shards:
        steps = jax.random.uniform(jax.random.fold_in(jax.random.fold_in(key, 6), position), (shards_of,), jnp.float32, least / len(shards), top_value / len(shards))
        factor_of = factor_of * jnp.repeat(jnp.exp(steps), dims[position] // shards_of).reshape((-1,) + (1,) * (len(dims) - 1 - position))
    return factor_of


def noise(stream_key, shape, width, bound, cuts=(), kind=jnp.bfloat16):
    drawn = jax.random.normal(stream_key, shape, jnp.float32) * width
    if len(cuts) > 0:
        drawn = levels(stream_key, shape, cuts, -0.22, 0.18) * drawn
    return jnp.clip(drawn, min=-bound, max=bound).astype(kind)


def bell_draw_with(key, shape, spread, bound, pieces, heavy, held_as=jnp.bfloat16):
    result = spread * jax.random.normal(key, shape, jnp.float32)
    if pieces:
        result = result * levels(key, shape, pieces, -0.22, 0.18)
    return jnp.clip(with_spikes(result, jax.random.fold_in(key, 3), *heavy), -bound, bound).astype(held_as)


def setup_inputs(seed: int = 0) -> dict:
    key_list = jax.random.split(jax.random.key(seed), 14)
    return {
        "context": bell_draw_with(key_list[0], (TOKENS, HEADS * HEAD_DIM), 1.0, 6.0, ((0, 16), (1, 8)), (0, 1, 16, 2.0)),
        "out_grad": noise(key_list[1], (TOKENS, D), 1.0, 6.0, ((0, 16), (1, 8))),
        "rewards": draw_rewards(jax.random.fold_in(key_list[13], 71), 0),
        "master": noise(key_list[3], (HEADS * HEAD_DIM, D), (HEADS * HEAD_DIM) ** -0.5, 0.078125, ((0, 16), (1, 8)), jnp.float32),
        "first_moment": noise(key_list[4], (HEADS * HEAD_DIM, D), (0.4 * (TOK_DEV * N_REP) ** -0.5), 0.03125, ((0, 16), (1, 8)), jnp.float32),
        "second_moment": jnp.clip(jnp.exp(math.log(3.0517578125e-05) - 4.6051702 * jax.random.uniform(key_list[5], (HEADS * HEAD_DIM, D), jnp.float32) ** levels(key_list[5], (HEADS * HEAD_DIM, D), ((0, 16), (1, 8)), -0.2, 0.2)), 3.0517577442878974e-07, 3.0517578125e-05),
        "inputs": noise(key_list[6], (STEPS, SEQS, D), 1.0, 6.0, ((1, 16),)),
        "w_query": noise(key_list[7], (D, HEADS * HEAD_DIM), D ** -0.5, 0.078125, ((1, 8),)),
        "w_key": noise(key_list[8], (D, KV_HEADS * HEAD_DIM), D ** -0.5, 0.078125, ((1, 8),)),
        "w_value": noise(key_list[9], (D, KV_HEADS * HEAD_DIM), D ** -0.5, 0.078125, ((1, 8),)),
        "cache_keys": draw_cache_keys(jax.random.fold_in(key_list[13], 71), 0),
        "cache_values": noise(key_list[11], (SEQS, CACHE, KV_HEADS * HEAD_DIM), 4.0, 24.0, ((0, 16), (2, 8))),
        "lengths": set_ends(jax.random.randint(key_list[12], (RPROMPTS,), CACHE // 4, CACHE + 1), jax.random.fold_in(key_list[12], 1), CACHE // 4, CACHE).astype(jnp.int32),
    }


rope_base = 1000000.0
first_beta = 0.9
second_beta = 0.95
adam_epsilon = 1e-08
step_count = 10
learn_rate = 0.001

def rotate(vectors, positions):
    half_dim = vectors.shape[-1] // 2
    frequency = rope_base ** (-2.0 * jnp.arange(half_dim, dtype=jnp.float32) / vectors.shape[-1])
    angles = positions[..., None].astype(jnp.float32) * frequency
    cosine_table = jnp.cos(angles)
    sine_table = jnp.sin(angles)
    former = vectors[..., :half_dim]
    latter = vectors[..., half_dim:]
    return jnp.concatenate([former * cosine_table - latter * sine_table, latter * cosine_table + former * sine_table], axis=-1)

def attend(queries, old_keys, old_values, new_keys, new_values, live_mask):
    score_scale = HEAD_DIM ** (-0.5)
    step_total = queries.shape[0]
    query_wide = queries.astype(jnp.float32)
    cache_scores = jnp.einsum('tsgqd,scgd->tsgqc', query_wide, old_keys.astype(jnp.float32)) * score_scale
    cache_scores = jnp.where(live_mask[None, :, None, None, :], cache_scores, -1e+30)
    recent = jnp.einsum('tsgqd,usgd->tsgqu', query_wide, new_keys.astype(jnp.float32)) * score_scale
    causal = jnp.arange(step_total)[:, None] >= jnp.arange(step_total)[None, :]
    recent = jnp.where(causal[:, None, None, None, :], recent, -1e+30)
    row_peak = jnp.maximum(lax.optimization_barrier(jnp.max(cache_scores, axis=-1)), lax.optimization_barrier(jnp.max(recent, axis=-1)))[..., None]
    cache_exp = jnp.exp(cache_scores - row_peak)
    recent_exp = jnp.exp(recent - row_peak)
    denominator = lax.optimization_barrier(jnp.sum(cache_exp, axis=-1, keepdims=True)) + lax.optimization_barrier(jnp.sum(recent_exp, axis=-1, keepdims=True))
    cache_weight = (cache_exp / denominator).astype(jnp.bfloat16)
    recent_weight = (recent_exp / denominator).astype(jnp.bfloat16)
    attended = jnp.einsum('tsgqc,scgd->tsgqd', cache_weight.astype(jnp.float32), old_values.astype(jnp.float32))
    attended = attended + jnp.einsum('tsgqu,usgd->tsgqd', recent_weight.astype(jnp.float32), new_values.astype(jnp.float32))
    return attended.astype(jnp.bfloat16)

def reference(context, out_grad, rewards, master, first_moment, second_moment, inputs, w_query, w_key, w_value, cache_keys, cache_values, lengths):
    group_size = rewards.shape[1]
    token_count = context.shape[0]
    totals = lax.optimization_barrier(jnp.sum(rewards.astype(jnp.float32), axis=1))
    advantage = rewards.astype(jnp.float32) - totals[:, None] / group_size
    ordered = advantage.reshape(PROMPTS_L, N_REP, GROUP_DEV).transpose(1, 0, 2).reshape(-1)
    per_token = jnp.repeat(ordered, RESP_LEN) / token_count
    scaled = (out_grad.astype(jnp.float32) * per_token[:, None]).astype(jnp.bfloat16)
    gradient = lax.dot_general(context, scaled, (((0,), (0,)), ((), ())), preferred_element_type=jnp.float32)
    moment_new = first_beta * first_moment + (1.0 - first_beta) * gradient
    square_new = second_beta * second_moment + (1.0 - second_beta) * gradient * gradient
    adam_step = moment_new / (1.0 - first_beta ** step_count) / (jnp.sqrt(square_new / (1.0 - second_beta ** step_count)) + adam_epsilon)
    weight = (master - learn_rate * adam_step).astype(jnp.bfloat16)
    step_total, seq_total, model_width = inputs.shape
    flat_rows = inputs.reshape(step_total * seq_total, model_width)
    queries = jnp.dot(flat_rows, w_query, preferred_element_type=jnp.float32).reshape(step_total, seq_total, HEADS, HEAD_DIM)
    key_new = jnp.dot(flat_rows, w_key, preferred_element_type=jnp.float32).reshape(step_total, seq_total, KV_HEADS, HEAD_DIM)
    value_new = jnp.dot(flat_rows, w_value, preferred_element_type=jnp.float32).reshape(step_total, seq_total, KV_HEADS, HEAD_DIM).astype(jnp.bfloat16)
    seq_length = jnp.repeat(lengths, ROLL_SAMP)
    positions = seq_length[None, :] + jnp.arange(step_total, dtype=jnp.int32)[:, None]
    queries = rotate(queries, positions[:, :, None]).astype(jnp.bfloat16)
    queries = queries.reshape(step_total, seq_total, KV_HEADS, HEADS // KV_HEADS, HEAD_DIM)
    key_new = rotate(key_new, positions[:, :, None]).astype(jnp.bfloat16)
    old_keys = cache_keys.reshape(seq_total, CACHE, KV_HEADS, HEAD_DIM)
    old_values = cache_values.reshape(seq_total, CACHE, KV_HEADS, HEAD_DIM)
    live_mask = jnp.arange(CACHE, dtype=jnp.int32)[None, :] < seq_length[:, None]
    attended = attend(queries, old_keys, old_values, key_new, value_new, live_mask)
    attended = attended.reshape(step_total * seq_total, HEADS * HEAD_DIM)
    decoded = jnp.dot(attended, weight, preferred_element_type=jnp.float32).astype(jnp.bfloat16)
    return (decoded.reshape(step_total, seq_total, model_width), adam_step)
```

```python
import functools
import jax
import jax.numpy as jnp
from jax import lax
from jax.experimental import pallas as pl
from jax.experimental.pallas import tpu as pltpu
from jax.sharding import PartitionSpec as P

MESH = pl.DeviceIdType.MESH
LANE = 128
CHUNKS = 5
HALF = 1024


def where_am_i():
    rep = lax.axis_index("rep")
    tp = lax.axis_index("tp")
    return rep // 4, (rep // 2) % 2, rep % 2, tp // 2, tp % 2


def device(x, yl, c, z, yh):
    return {"rep": (x * 2 + yl) * 2 + c, "tp": z * 2 + yh}


def gradient_kernel(
    ctx, outg, rewards, counts, grad,
    cb, sr, relay, ss, tot, totf, keep, give, got, part, xb, tb, ob,
    load_sem, c_send, c_recv, f_send, f_recv, s_send, r_recv, r_send, p_recv,
    t_send, t_recv, d_send, d_recv, x_send, x_recv, o_send, o_recv,
):
    x, yl, c, z, yh = where_am_i()
    rep = lax.axis_index("rep")
    tp = lax.axis_index("tp")
    y = yh * 2 + yl
    yp, ym = (y + 1) % 4, (y + 3) % 4
    z_up = device(x, yl, c, (z + 1) % 4, yh)
    z_dn = device(x, yl, c, (z + 3) % 4, yh)
    y_up = device(x, yp % 2, c, z, yp // 2)
    y_dn = device(x, ym % 2, c, z, ym // 2)
    mate = device(x, yl, 1 - c, z, yh)

    def load(src, dst, j, k):
        return pltpu.make_async_copy(src.at[:, pl.ds(j * LANE, LANE)], dst, load_sem.at[k, j])

    for j in range(CHUNKS):
        load(ctx, cb.at[0, j], j, 0).start()
        load(outg, sr.at[0, j], j, 1).start()

    barrier = pltpu.get_barrier_semaphore()

    def greet(target):
        pl.semaphore_signal(barrier, inc=1, device_id=target, device_id_type=MESH)

    @pl.loop(1, 16)
    def _(d):
        greet({"rep": (rep + d) % 16, "tp": tp})

    for k in range(4):
        greet(device(x, k // 2, k % 2, z, 1 - yh))
    greet(z_up)
    greet(z_dn)
    pl.semaphore_wait(barrier, 21)

    def send(src, dst, ss_, rs_, target):
        return pltpu.make_async_remote_copy(
            src_ref=src, dst_ref=dst, send_sem=ss_, recv_sem=rs_,
            device_id=target, device_id_type=MESH,
        )

    tot[0] = counts[...]

    def count_copy(d):
        return send(counts, tot.at[d], t_send.at[d], t_recv.at[d], {"rep": (rep + d) % 16, "tp": tp})

    @pl.loop(1, 16)
    def _(d):
        count_copy(d).start()

    def own_up(j):
        return send(cb.at[0, j], cb.at[1, j], c_send.at[0, j], c_recv.at[0, j], z_up)

    def own_dn(j):
        return send(cb.at[0, j], cb.at[3, j], c_send.at[1, j], c_recv.at[1, j], z_dn)

    first, second = pl.ds(0, HALF), pl.ds(HALF, HALF)

    def fwd_up(j):
        return send(cb.at[1, j, first], cb.at[2, j, first], f_send.at[0, j], f_recv.at[0, j], z_up)

    def fwd_dn(j):
        return send(cb.at[3, j, second], cb.at[2, j, second], f_send.at[1, j], f_recv.at[1, j], z_dn)

    def out_up(j):
        return send(sr.at[0, j, first], relay.at[0, j], s_send.at[0, j], r_recv.at[0, j], y_up)

    def out_dn(j):
        return send(sr.at[0, j, second], relay.at[1, j], s_send.at[1, j], r_recv.at[1, j], y_dn)

    def pass_up(j):
        return send(relay.at[0, j], sr.at[1, j, first], r_send.at[0, j], p_recv.at[0, j], y_up)

    def pass_dn(j):
        return send(relay.at[1, j], sr.at[1, j, second], r_send.at[1, j], p_recv.at[1, j], y_dn)

    def issue(j):
        own_up(j).start()
        own_dn(j).start()
        out_up(j).start()
        out_dn(j).start()

    for j in range(CHUNKS):
        load(ctx, cb.at[0, j], j, 0).wait()
        load(outg, sr.at[0, j], j, 1).wait()
        if j < 2:
            issue(j)

    @pl.loop(1, 16)
    def _(d):
        count_copy(d).wait()

    totf[...] = jnp.sum(tot[...], axis=0) * (1.0 / 64.0)

    def scale(rel):
        @pl.loop(0, 32)
        def _(seg):
            rows = pl.ds(pl.multiple_of(seg * 64, 64), 64)
            p = seg // 4
            factor = (rewards[p, seg % 4].astype(jnp.float32) - totf[pl.ds(p, 1), :]) * (1.0 / 32768.0)
            for j in range(CHUNKS):
                ss[rel, rows, j * LANE : (j + 1) * LANE] = (
                    sr[rel, j, rows, :].astype(jnp.float32) * factor
                ).astype(jnp.bfloat16)

    scale(0)

    def step(j):
        own_up(j).wait_recv()
        fwd_up(j).start()
        own_dn(j).wait_recv()
        fwd_dn(j).start()
        out_up(j).wait_recv()
        pass_up(j).start()
        out_dn(j).wait_recv()
        pass_dn(j).start()
        if j + 2 < CHUNKS:
            issue(j + 2)

    def far(j):
        fwd_up(j).wait_recv()
        fwd_dn(j).wait_recv()

    def keeps(rel):
        s = yh if rel == 0 else 1 - yh
        return c == s

    def hand(j, r):
        return send(give.at[j, r], got.at[j, r], d_send.at[j, r], d_recv.at[j, r], mate)

    def compute(j, rel):
        mine = keeps(rel)

        @pl.loop(0, 4)
        def _(r):
            block = lax.dot_general(
                cb[r, j], ss[rel], (((0,), (0,)), ((), ())), preferred_element_type=jnp.float32
            )

            @pl.when(mine)
            def _():
                keep[j, r] = block

            @pl.when(jnp.logical_not(mine))
            def _():
                give[j, r] = block.astype(jnp.bfloat16)
                hand(j, r).start()

    def over_x(j, dx):
        to = (x + dx) % 4
        r = (z - to + 4) % 4
        return send(part.at[j, r], xb.at[j, dx - 1], x_send.at[j, dx - 1], x_recv.at[j, dx - 1],
                    device(to, yl, c, z, yh))

    def pair_sum(j, rel):
        @pl.when(keeps(rel))
        def _():
            @pl.loop(0, 4)
            def _(r):
                hand(j, r).wait_recv()
                part[j, r] = (keep[j, r] + got[j, r].astype(jnp.float32)).astype(jnp.bfloat16)

            for dx in (2, 1, 3):
                over_x(j, dx).start()

    def pieces(j):
        if j < 2:
            return ((0, 128, 0, 128 * j, j),)
        if j > 2:
            return ((0, 128, 1, 128 * j - 320, j - 2),)
        return ((0, 64, 0, 256, 2), (64, 64, 1, 0, 0))

    def to_owner(j, piece, local):
        at, rows, core, row, k = piece
        src = tb.at[j, pl.ds(at, rows)]
        dst = ob.at[yl, pl.ds(row, rows)]
        if local:
            return pltpu.make_async_copy(src, dst, o_recv.at[yl, k])
        return send(src, dst, o_send.at[j, at // 64], o_recv.at[yl, k], device(x, yh, core, z, c))

    def is_me(core):
        return jnp.logical_and(jnp.logical_and(c == yh, yh == yl), c == core)

    def x_sum(j, rel):
        @pl.when(keeps(rel))
        def _():
            total = part[j, (z - x + 4) % 4].astype(jnp.float32)
            for dx in (1, 2, 3):
                over_x(j, dx).wait_recv()
                total = total + xb[j, dx - 1].astype(jnp.float32)
            tb[j] = total.astype(jnp.bfloat16)
            for piece in pieces(j):
                @pl.when(is_me(piece[2]))
                def _():
                    to_owner(j, piece, True).start()

                @pl.when(jnp.logical_not(is_me(piece[2])))
                def _():
                    to_owner(j, piece, False).start()

    step(0)
    step(1)
    far(0)
    compute(0, 0)
    step(2)
    pair_sum(0, 0)
    far(1)
    compute(1, 0)
    pair_sum(1, 0)
    step(3)
    x_sum(0, 0)
    step(4)
    for j in range(CHUNKS):
        pass_up(j).wait_recv()
        pass_dn(j).wait_recv()
    scale(1)
    compute(0, 1)
    compute(1, 1)
    pair_sum(0, 1)
    far(2)
    compute(2, 0)
    pair_sum(1, 1)
    x_sum(1, 0)
    compute(2, 1)
    pair_sum(2, 0)
    x_sum(0, 1)
    pair_sum(2, 1)
    far(3)
    compute(3, 0)
    x_sum(1, 1)
    compute(3, 1)
    pair_sum(3, 0)
    x_sum(2, 0)
    pair_sum(3, 1)
    x_sum(2, 1)
    far(4)
    compute(4, 0)
    compute(4, 1)
    pair_sum(4, 0)
    pair_sum(4, 1)
    x_sum(3, 0)
    x_sum(3, 1)
    x_sum(4, 0)
    x_sum(4, 1)

    sizes0 = (128, 128, 64)
    rows0 = (0, 128, 256)
    sizes1 = (64, 128, 128)
    rows1 = (0, 64, 192)
    for core, sizes, starts in ((0, sizes0, rows0), (1, sizes1, rows1)):
        @pl.when(c == core)
        def _():
            for src in range(2):
                for k in range(3):
                    there = ob.at[src, pl.ds(starts[k], sizes[k])]
                    pltpu.make_async_copy(there, there, o_recv.at[src, k]).wait()

    grad[...] = ob[0].astype(jnp.float32) + ob[1].astype(jnp.float32)

    for j in range(CHUNKS):
        for copy in (own_up(j), own_dn(j), fwd_up(j), fwd_dn(j), out_up(j), out_dn(j), pass_up(j), pass_dn(j)):
            copy.wait_send()

        @pl.loop(0, 4)
        def _(r):
            hand(j, r).wait_send()

        for dx in (1, 2, 3):
            over_x(j, dx).wait_send()
        for piece in pieces(j):
            @pl.when(jnp.logical_not(is_me(piece[2])))
            def _():
                to_owner(j, piece, False).wait_send()


def gradient_of(context, out_grad, rewards, counts):
    bf, f32 = jnp.bfloat16, jnp.float32
    dma = pltpu.SemaphoreType.DMA
    tokens, width = context.shape
    return pl.pallas_call(
        gradient_kernel,
        out_shape=jax.ShapeDtypeStruct((320, width), f32),
        in_specs=[
            pl.BlockSpec(memory_space=pl.ANY),
            pl.BlockSpec(memory_space=pl.ANY),
            pl.BlockSpec(memory_space=pltpu.SMEM),
            pl.BlockSpec(memory_space=pltpu.VMEM),
        ],
        out_specs=pl.BlockSpec(memory_space=pltpu.VMEM),
        scratch_shapes=[
            pltpu.VMEM((4, CHUNKS, tokens, LANE), bf),
            pltpu.VMEM((2, CHUNKS, tokens, LANE), bf),
            pltpu.VMEM((2, CHUNKS, HALF, LANE), bf),
            pltpu.VMEM((2, tokens, width), bf),
            pltpu.VMEM((16, 8, LANE), f32),
            pltpu.VMEM((8, LANE), f32),
            pltpu.VMEM((CHUNKS, 4, LANE, width), f32),
            pltpu.VMEM((CHUNKS, 4, LANE, width), bf),
            pltpu.VMEM((CHUNKS, 4, LANE, width), bf),
            pltpu.VMEM((CHUNKS, 4, LANE, width), bf),
            pltpu.VMEM((CHUNKS, 3, LANE, width), bf),
            pltpu.VMEM((CHUNKS, LANE, width), bf),
            pltpu.VMEM((2, 320, width), bf),
            dma((2, CHUNKS)),
            dma((2, CHUNKS)), dma((2, CHUNKS)),
            dma((2, CHUNKS)), dma((2, CHUNKS)),
            dma((2, CHUNKS)), dma((2, CHUNKS)),
            dma((2, CHUNKS)), dma((2, CHUNKS)),
            dma((16,)), dma((16,)),
            dma((CHUNKS, 4)), dma((CHUNKS, 4)),
            dma((CHUNKS, 3)), dma((CHUNKS, 3)),
            dma((CHUNKS, 2)), dma((2, 3)),
        ],
        compiler_params=pltpu.CompilerParams(
            collective_id=0, has_side_effects=True, vmem_limit_bytes=60 * 1024 * 1024
        ),
        cost_estimate=pl.CostEstimate(flops=13_400_000_000, bytes_accessed=6_000_000, transcendentals=0),
        name="gradient",
    )(context, out_grad, rewards, counts)


HEAD_DIM = 128


rope_base = 1000000.0
first_beta = 0.9
second_beta = 0.95
adam_epsilon = 1e-08
step_count = 10
learn_rate = 0.001


def from_everyone(array, axis):
    devices = lax.axis_size(axis)
    return lax.all_to_all(
        jnp.broadcast_to(array[None], (devices, *array.shape)), axis, 0, 0, tiled=True
    )


def of_everyone(array, axis):
    everything = from_everyone(array, axis)
    return jnp.sum(everything, axis=0)


def laid_out(tiles, dim):
    tiles = jnp.moveaxis(tiles, 0, dim)
    lengths = tiles.shape
    return tiles.reshape(*lengths[:dim], lengths[dim] * lengths[dim + 1], *lengths[dim + 2 :])


def collect(array, axis, dim):
    return laid_out(from_everyone(array, axis), dim)


def split_up(array, dim, devices):
    before, after = (array.shape[:dim], array.shape[dim + 1 :])
    return jnp.moveaxis(array.reshape(*before, devices, -1, *after), dim, 0)


def sum_at_owner(array, axis, dim):
    tiles = split_up(array, dim, lax.axis_size(axis))
    arrived = lax.all_to_all(tiles, axis, split_axis=0, concat_axis=0, tiled=True)
    return arrived.sum(axis=0)


def rotate(vectors, positions):
    half_dim = vectors.shape[-1] // 2
    frequency = rope_base ** (-2.0 * jnp.arange(half_dim, dtype=jnp.float32) / vectors.shape[-1])
    angles = positions[..., None].astype(jnp.float32) * frequency
    cosine_table = jnp.cos(angles)
    sine_table = jnp.sin(angles)
    former = vectors[..., :half_dim]
    latter = vectors[..., half_dim:]
    return jnp.concatenate(
        [former * cosine_table - latter * sine_table, latter * cosine_table + former * sine_table],
        axis=-1,
    )


def attend(queries, old_keys, old_values, new_keys, new_values, live_mask):
    score_scale = HEAD_DIM ** (-0.5)
    step_total = queries.shape[0]
    cache_scores = (
        jnp.einsum("tsgqd,scgd->tsgqc", queries, old_keys, preferred_element_type=jnp.float32)
        * score_scale
    )
    cache_scores = jnp.where(live_mask[None, :, None, None, :], cache_scores, -1e30)
    recent = (
        jnp.einsum("tsgqd,usgd->tsgqu", queries, new_keys, preferred_element_type=jnp.float32)
        * score_scale
    )
    causal = jnp.arange(step_total)[:, None] >= jnp.arange(step_total)[None, :]
    recent = jnp.where(causal[:, None, None, None, :], recent, -1e30)
    row_peak = jnp.maximum(jnp.max(cache_scores, axis=-1), jnp.max(recent, axis=-1))[..., None]
    cache_exp = jnp.exp(cache_scores - row_peak)
    recent_exp = jnp.exp(recent - row_peak)
    denominator = jnp.sum(cache_exp, axis=-1, keepdims=True) + jnp.sum(
        recent_exp, axis=-1, keepdims=True
    )
    cache_weight = (cache_exp / denominator).astype(jnp.bfloat16)
    recent_weight = (recent_exp / denominator).astype(jnp.bfloat16)
    attended = jnp.einsum(
        "tsgqc,scgd->tsgqd", cache_weight, old_values, preferred_element_type=jnp.float32
    )
    attended = attended + jnp.einsum(
        "tsgqu,usgd->tsgqd", recent_weight, new_values, preferred_element_type=jnp.float32
    )
    return attended.astype(jnp.bfloat16)


def per_device(
    context,
    out_grad,
    rewards,
    master,
    first_moment,
    second_moment,
    inputs,
    w_query,
    w_key,
    w_value,
    cache_keys,
    cache_values,
    lengths,
):
    counts = jnp.broadcast_to(
        jnp.sum(rewards, axis=1).astype(jnp.float32)[:, None], (rewards.shape[0], LANE)
    )
    gradient = gradient_of(context, out_grad, rewards, counts)
    moment_new = first_beta * first_moment + (1.0 - first_beta) * gradient
    square_new = second_beta * second_moment + (1.0 - second_beta) * gradient * gradient
    adam_step = (
        moment_new
        / (1.0 - first_beta**step_count)
        / (jnp.sqrt(square_new / (1.0 - second_beta**step_count)) + adam_epsilon)
    )
    weight = (master - learn_rate * adam_step).astype(jnp.bfloat16)
    step_total, seq_local, model_width = inputs.shape
    local_heads = w_query.shape[1] // HEAD_DIM
    local_kv = w_key.shape[1] // HEAD_DIM
    flat_rows = inputs.reshape(step_total * seq_local, model_width)
    queries = jnp.dot(flat_rows, w_query, preferred_element_type=jnp.float32).reshape(
        step_total, seq_local, local_heads, HEAD_DIM
    )
    key_new = jnp.dot(flat_rows, w_key, preferred_element_type=jnp.float32).reshape(
        step_total, seq_local, local_kv, HEAD_DIM
    )
    value_new = (
        jnp.dot(flat_rows, w_value, preferred_element_type=jnp.float32)
        .reshape(step_total, seq_local, local_kv, HEAD_DIM)
        .astype(jnp.bfloat16)
    )
    seq_length = jnp.repeat(lengths, seq_local // lengths.shape[0])
    positions = seq_length[None, :] + jnp.arange(step_total, dtype=jnp.int32)[:, None]
    queries = rotate(queries, positions[:, :, None]).astype(jnp.bfloat16)
    queries = queries.reshape(step_total, seq_local, local_kv, local_heads // local_kv, HEAD_DIM)
    key_new = rotate(key_new, positions[:, :, None]).astype(jnp.bfloat16)
    slot_total = cache_keys.shape[1]
    old_keys = cache_keys.reshape(seq_local, slot_total, local_kv, HEAD_DIM)
    old_values = cache_values.reshape(seq_local, slot_total, local_kv, HEAD_DIM)
    live_mask = jnp.arange(slot_total, dtype=jnp.int32)[None, :] < seq_length[:, None]
    attended = attend(queries, old_keys, old_values, key_new, value_new, live_mask)
    attended = attended.reshape(step_total * seq_local, local_heads * HEAD_DIM)
    all_heads = collect(attended, "tp", 1)
    feature_rows = lax.all_to_all(all_heads, "rep", split_axis=1, concat_axis=0, tiled=True)
    own_columns = sum_at_owner(
        jnp.dot(feature_rows, weight, preferred_element_type=jnp.float32), "rep", 0
    )
    decoded = collect(own_columns.astype(jnp.bfloat16), "tp", 1)
    return (decoded.reshape(step_total, seq_local, model_width), adam_step)


def solution(mesh):
    placed = (
        P("rep", "tp"),
        P("rep", "tp"),
        P(None, "rep"),
        P("rep", "tp"),
        P("rep", "tp"),
        P("rep", "tp"),
        P(None, "rep", None),
        P(None, "tp"),
        P(None, "tp"),
        P(None, "tp"),
        P("rep", None, "tp"),
        P("rep", None, "tp"),
        P("rep"),
    )
    return jax.shard_map(
        per_device,
        mesh=mesh,
        in_specs=placed,
        out_specs=(P(None, "rep", None), P("rep", "tp")),
        check_vma=False,
    )
```

```python
import jax
import jax.numpy as jnp
from jax import lax
from jax.experimental import pallas as pl
from jax.experimental.pallas import tpu as pltpu
from jax.sharding import PartitionSpec as P

HEAD_DIM = 128

rope_base = 1000000.0
first_beta = 0.9
second_beta = 0.95
adam_epsilon = 1e-08
step_count = 10
learn_rate = 0.001

MESH = pl.DeviceIdType.MESH
LANE = 128
CHUNKS = 5
HALF = 1024
SPANS = ((0, 3), (3, 2))
ROWS = 320
BF, F32 = jnp.bfloat16, jnp.float32


def device(x, yl, c, z, yh):
    return {"rep": (x * 2 + yl) * 2 + c, "tp": z * 2 + yh}


def step_kernel(
    ctx, outg, rewards, counts, heads, master, first_m, second_m,
    adam, decoded,
    cb, sr, ss, tot, totf, keep, give, got, part, xb, tb, ob,
    ag, hx, ab, aa, wb, dgive, dgot, dpart, dxb, dkeep, dys, dyb, dec,
    load_sem, c_send, c_recv, f_send, f_recv, s_send, s_recv,
    t_send, t_recv, d_send, d_recv, x_send, x_recv, o_send, o_recv,
    g_send, g_recv, i_send, i_recv, a_send, a_recv,
    e_send, e_recv, h_send, h_recv, y_send, y_recv, l_send, l_recv,
):
    rep = lax.axis_index("rep")
    tp = lax.axis_index("tp")
    x, yl, c, z, yh = rep // 4, (rep // 2) % 2, rep % 2, tp // 2, tp % 2
    z_up = device(x, yl, c, (z + 1) % 4, yh)
    z_dn = device(x, yl, c, (z + 3) % 4, yh)
    across = device(x, yl, c, z, 1 - yh)
    mate = device(x, yl, 1 - c, z, yh)
    beside = device(x, 1 - yl, c, z, yh)

    def load(src, dst, j, k):
        return pltpu.make_async_copy(src.at[:, pl.ds(j * LANE, LANE)], dst, load_sem.at[k, j])

    for j in range(CHUNKS):
        load(ctx, cb.at[0, j], j, 0).start()
        load(outg, sr.at[0, j], j, 1).start()

    barrier = pltpu.get_barrier_semaphore()

    def greet(target):
        pl.semaphore_signal(barrier, inc=1, device_id=target, device_id_type=MESH)

    @pl.loop(1, 32)
    def _(d):
        e = (rep * 2 + yh + d) % 32
        greet({"rep": e // 2, "tp": z * 2 + e % 2})

    @pl.loop(0, 6)
    def _(d):
        greet({"rep": rep, "tp": (z * 2 + 2 + d) % 8})

    pl.semaphore_wait(barrier, 37)

    def send(src, dst, ss_, rs_, target):
        return pltpu.make_async_remote_copy(
            src_ref=src, dst_ref=dst, send_sem=ss_, recv_sem=rs_,
            device_id=target, device_id_type=MESH,
        )

    first, second = pl.ds(0, HALF), pl.ds(HALF, HALF)

    def own_up(j):
        return send(cb.at[0, j], cb.at[1, j], c_send.at[0, j], c_recv.at[0, j], z_up)

    def own_dn(j):
        return send(cb.at[0, j], cb.at[3, j], c_send.at[1, j], c_recv.at[1, j], z_dn)

    def fwd_up(j):
        return send(cb.at[1, j, first], cb.at[2, j, first], f_send.at[0, j], f_recv.at[0, j], z_up)

    def fwd_dn(j):
        return send(cb.at[3, j, second], cb.at[2, j, second], f_send.at[1, j], f_recv.at[1, j], z_dn)

    def trade(j):
        return send(sr.at[0, j], sr.at[1, j], s_send.at[j], s_recv.at[j], across)

    def heads_z(dz):
        return send(heads, ag.at[dz], g_send.at[dz], g_recv.at[dz], device(x, yl, c, (z + dz) % 4, yh))

    @pl.loop(1, 4)
    def _(dz):
      heads_z(dz).start()

    for j in range(CHUNKS):
        load(ctx, cb.at[0, j], j, 0).wait()
        if j < 2:
            own_up(j).start()
            own_dn(j).start()
        load(outg, sr.at[0, j], j, 1).wait()
        if j < 2: trade(j).start()

    tot[0] = counts[...]

    def count_copy(d):
        return send(counts, tot.at[d], t_send.at[d], t_recv.at[d], {"rep": (rep + d) % 16, "tp": tp})

    @pl.loop(1, 16)
    def _(d):
        count_copy(d).start()

    @pl.loop(1, 16)
    def _(d):
        count_copy(d).wait()

    totf[...] = jnp.sum(tot[...], axis=0) * (1.0 / 64.0)

    def scale(rel):
        @pl.loop(0, 32)
        def _(seg):
            rows = pl.ds(pl.multiple_of(seg * 64, 64), 64)
            p = seg // 4
            factor = (rewards[p, seg % 4].astype(F32) - totf[pl.ds(p, 1), :]) * (1.0 / 32768.0)
            for j in range(CHUNKS):
                ss[rel, rows, j * LANE : (j + 1) * LANE] = (
                    sr[rel, j, rows, :].astype(F32) * factor
                ).astype(BF)

    scale(0)

    def step(j):
        own_up(j).wait_recv()
        fwd_up(j).start()
        own_dn(j).wait_recv()
        fwd_dn(j).start()
        if j + 2 < CHUNKS:
            own_up(j + 2).start()
            own_dn(j + 2).start()
        if j + 2 < CHUNKS:
            trade(j + 2).start()

    def far(j):
        fwd_up(j).wait_recv()
        fwd_dn(j).wait_recv()

    def hand(j, r):
        return send(give.at[j, r], got.at[j, r], d_send.at[j, r], d_recv.at[j, r], mate)

    def over_x(j, r, dx):
        slot = (dx + 3) % 4
        return send(part.at[j, r], xb.at[j, slot], x_send.at[j, slot], x_recv.at[j, slot],
                    device((x + dx) % 4, yl, c, z, yh))

    def contribute(low, high, rels):
        count = (high - low) * len(rels)

        def task(n):
            i = low + n // len(rels)
            rel = rels[0] + n % len(rels)
            rr = i % 4
            return i // 4, rr ^ (rr // 2), rel, (yh + rel) % 2 == c

        def compute(n):
            j, r, rel, mine = task(n)
            block = lax.dot_general(
                cb[r, j], ss[rel], (((0,), (0,)), ((), ())), preferred_element_type=F32
            )

            @pl.when(mine)
            def _():
                keep[n // len(rels)] = block

            @pl.when(jnp.logical_not(mine))
            def _():
                give[j, r] = block.astype(BF)
                hand(j, r).start()

        def pair(n):
            j, r, rel, mine = task(n)

            @pl.when(mine)
            def _():
                hand(j, r).wait_recv()
                part[j, r] = (keep[n // len(rels)] + got[j, r].astype(F32)).astype(BF)
                dx = (z - r - x + 8) % 4

                @pl.when(dx != 0)
                def _():
                    over_x(j, r, dx).start()

        @pl.loop(0, count + 2)
        def _(n):
            @pl.when(n < count)
            def _():
                compute(n)

            @pl.when(n >= 2)
            def _():
                pair(n - 2)

    def pieces(j):
        if j < 2:
            return ((0, 128, 0, 128 * j, j),)
        if j > 2:
            return ((0, 128, 1, 128 * j - ROWS, j - 2),)
        return ((0, 64, 0, 256, 2), (64, 64, 1, 0, 0))

    def to_owner(j, piece, local):
        at, rows, core, row, k = piece
        src = tb.at[j, pl.ds(at, rows)]
        dst = ob.at[yl, pl.ds(row, rows)]
        if local:
            return pltpu.make_async_copy(src, dst, o_recv.at[yl, k])
        return send(src, dst, o_send.at[j, at // 64], o_recv.at[yl, k], device(x, yh, core, z, c))

    def is_me(core):
        return jnp.logical_and(jnp.logical_and(c == yh, yh == yl), c == core)

    def x_sum(j):
        total = part[j, (z - x + 4) % 4].astype(F32)
        for slot in range(3):
            over_x(j, 0, slot + 1).wait_recv()
            total = total + xb[j, slot].astype(F32)
        tb[j] = total.astype(BF)
        for piece in pieces(j):
            @pl.when(is_me(piece[2]))
            def _():
                to_owner(j, piece, True).start()

            @pl.when(jnp.logical_not(is_me(piece[2])))
            def _():
                to_owner(j, piece, False).start()

    def heads_x(dz, local):
        to = (z - dz + 4) % 4
        if local:
            return pltpu.make_async_copy(ag.at[dz], hx.at[x], i_recv.at[x])
        return send(ag.at[dz], hx.at[x], i_send.at[dz], i_recv.at[x], device(to, yl, c, z, yh))

    def stays_x(dz):
        return (z - dz + 4) % 4 == x

    def heads_over_x():
        ag[0] = heads[...]
        for dz in (1, 2, 3):
            heads_z(dz).wait_recv()

        @pl.loop(0, 4)
        def _(dz):
            @pl.when(stays_x(dz))
            def _():
                heads_x(dz, True).start()

            @pl.when(jnp.logical_not(stays_x(dz)))
            def _():
                heads_x(dz, False).start()

    def spread(h, other, local):
        src = hx.at[:, pl.ds(h * ROWS, ROWS)]
        dst = ab.at[yl * 2 + c]
        if local:
            return pltpu.make_async_copy(src, dst, a_recv.at[yl * 2 + c])
        return send(src, dst, a_send.at[h, other], a_recv.at[yl * 2 + c], device(x, yh, h, z, other))

    def stays(h, other):
        return jnp.logical_and(yh == yl, jnp.logical_and(h == c, other == yh))

    def spread_heads():

        @pl.loop(0, 4)
        def _(k):
            pltpu.make_async_copy(hx.at[k], hx.at[k], i_recv.at[k]).wait()

        for h in range(2):
            for other in range(2):
                @pl.when(stays(h, other))
                def _():
                    spread(h, other, True).start()

                @pl.when(jnp.logical_not(stays(h, other)))
                def _():
                    spread(h, other, False).start()

    def take_heads():
        for k in range(4):
            pltpu.make_async_copy(ab.at[k], ab.at[k], a_recv.at[k]).wait()

        @pl.loop(0, 16)
        def _(g):
            aa[g] = ab[g // 4, g % 4].T

    step(0)
    contribute(0, 3, (0,))
    heads_over_x()
    step(1)
    contribute(4, 7, (0,))
    far(0)
    contribute(3, 4, (0,))
    step(2)
    contribute(8, 11, (0,))
    far(1)
    contribute(7, 8, (0,))
    step(3)
    contribute(12, 15, (0,))
    for j in range(CHUNKS):
        trade(j).wait_recv()
    spread_heads()
    scale(1)
    contribute(0, 11, (1,))
    far(2)
    contribute(11, 12, (0, 1))
    contribute(12, 15, (1,))
    step(4)
    contribute(16, 19, (0, 1))
    x_sum(0)
    x_sum(1)
    far(3)
    contribute(15, 16, (0, 1))
    x_sum(2)
    take_heads()
    far(4)
    contribute(19, 20, (0, 1))
    x_sum(3)
    x_sum(4)

    for core, sizes, starts in ((0, (128, 128, 64), (0, 128, 256)), (1, (64, 128, 128), (0, 64, 192))):
        @pl.when(c == core)
        def _():
            for src in range(2):
                for k in range(3):
                    there = ob.at[src, pl.ds(starts[k], sizes[k])]
                    pltpu.make_async_copy(there, there, o_recv.at[src, k]).wait()

    @pl.loop(0, ROWS // 32)
    def _(n):
        rows = pl.ds(pl.multiple_of(n * 32, 32), 32)
        gradient = ob[0, rows, :].astype(F32) + ob[1, rows, :].astype(F32)
        moment_new = first_beta * first_m[rows, :] + (1.0 - first_beta) * gradient
        square_new = second_beta * second_m[rows, :] + (1.0 - second_beta) * gradient * gradient
        direction = (
            moment_new
            / (1.0 - first_beta**step_count)
            / (jnp.sqrt(square_new / (1.0 - second_beta**step_count)) + adam_epsilon)
        )
        adam[rows, :] = direction
        wb[rows, :] = (master[rows, :] - learn_rate * direction).astype(BF)

    def blocks(q):
        return pl.ds(*SPANS[q])

    def d_hand(q, xg):
        return send(dgive.at[xg, :, blocks(q)], dgot.at[xg, :, blocks(q)], e_send.at[q, xg], e_recv.at[q, xg], mate)

    def d_over_x(q, dx):
        slot = (dx + 3) % 4
        to = (x + dx) % 4
        return send(dpart.at[to, :, blocks(q)], dxb.at[slot, :, blocks(q)], h_send.at[q, slot], h_recv.at[q, slot],
                    device(to, yl, c, z, yh))

    def d_beside(q):
        return send(dys.at[blocks(q)], dyb.at[blocks(q)], y_send.at[q], y_recv.at[q], beside)

    def d_across(q):
        there = dec.at[tp, blocks(q)]
        return send(there, there, l_send.at[q, 0], l_recv.at[q, tp], across)

    def d_over_z(q, dz, other):
        mine = z * 2 + (1 - yh if other else yh)
        there = dec.at[mine, blocks(q)]
        return send(there, there, l_send.at[q, dz + 3 * other], l_recv.at[q, mine],
                    device(x, yl, c, (z + dz) % 4, yh))

    def d_multiply(q):
        start, width = SPANS[q]
        columns = slice(start * LANE, (start + width) * LANE)

        @pl.loop(0, 8)
        def _(n):
            xg, side = (x + n // 2 + 2) % 4, n % 2
            block = jnp.dot(aa[side * 8 + (1 - c) * 4 + xg], wb[:, columns], preferred_element_type=F32)
            for b in range(width):
                dgive[xg, side, start + b] = block[:, b * LANE : (b + 1) * LANE].astype(BF)

            @pl.when(side == 1)
            def _():
                d_hand(q, xg).start()

        @pl.loop(0, 8)
        def _(n):
            dx, side = (n // 2 + 2) % 4, n % 2
            xg = (x + dx) % 4
            block = jnp.dot(aa[side * 8 + c * 4 + xg], wb[:, columns], preferred_element_type=F32)

            @pl.when(side == 0)
            def _():
                d_hand(q, xg).wait_recv()

            for b in range(width):
                dpart[xg, side, start + b] = (
                    block[:, b * LANE : (b + 1) * LANE] + dgot[xg, side, start + b].astype(F32)
                ).astype(BF)

            if q == 0:
                @pl.when(jnp.logical_and(side == 1, dx != 0))
                def _():
                    d_over_x(q, dx).start()

    def d_x_sum(q):
        start, width = SPANS[q]
        for dx in (1, 3, 2):
            d_over_x(q, dx).wait_recv()

        def total(side, b):
            value = dpart[x, side, b].astype(F32)
            for slot in range(3):
                value = value + dxb[slot, side, b].astype(F32)
            return value

        for b in range(start, start + width):
            dys[b] = total(1 - yl, b).astype(BF)
        d_beside(q).start()
        for b in range(start, start + width):
            dkeep[b] = total(yl, b)

    def d_finish(q):
        start, width = SPANS[q]
        d_beside(q).wait_recv()
        for b in range(start, start + width):
            dec[tp, b] = (dkeep[b] + dyb[b].astype(F32)).astype(BF)
        for dz in (2, 1, 3):
            d_over_z(q, dz, 0).start()
        d_across(q).start()

    def d_pass(q):
        other = dec.at[z * 2 + 1 - yh, blocks(q)]
        pltpu.make_async_copy(other, other, l_recv.at[q, z * 2 + 1 - yh]).wait()
        for dz in (2, 1, 3):
            d_over_z(q, dz, 1).start()

    d_multiply(0)
    if len(SPANS) > 1:
        d_multiply(1)
    d_x_sum(0)
    if len(SPANS) > 1:
        for dx in (2, 1, 3):
            d_over_x(1, dx).start()
    d_finish(0)
    d_pass(0)
    if len(SPANS) > 1:
        d_x_sum(1)
        d_finish(1)
        d_pass(1)

    for q in range(len(SPANS)):
        start, width = SPANS[q]

        @pl.loop(2, 8)
        def _(d):
            t = (z * 2 + d) % 8
            pltpu.make_async_copy(dec.at[t, blocks(q)], dec.at[t, blocks(q)], l_recv.at[q, t]).wait()

        for t in range(8):
            for b in range(start, start + width):
                decoded[:, t * 640 + b * LANE : t * 640 + (b + 1) * LANE] = dec[t, b]

    for j in range(CHUNKS):
        for copy in (own_up(j), own_dn(j), fwd_up(j), fwd_dn(j)) + (trade(j),):
            copy.wait_send()

        @pl.loop(0, 4)
        def _(r):
          hand(j, r).wait_send()

        if j < len(SPANS):
          @pl.loop(0, 4)
          def _(k):
            d_hand(j, k).wait_send()

          d_beside(j).wait_send()
          d_across(j).wait_send()
          for dz in (1, 2, 3):
            d_over_x(j, dz).wait_send()
            d_over_z(j, dz, 0).wait_send()
            d_over_z(j, dz, 1).wait_send()

        for dx in (1, 2, 3):
            over_x(j, 0, dx).wait_send()
        for piece in pieces(j):
          @pl.when(jnp.logical_not(is_me(piece[2])))
          def _():
              to_owner(j, piece, False).wait_send()

    for dz in (1, 2, 3):
      heads_z(dz).wait_send()

    @pl.loop(0, 4)
    def _(dz):
      @pl.when(jnp.logical_not(stays_x(dz)))
      def _():
          heads_x(dz, False).wait_send()

    for h in range(2):
      for other in range(2):
          @pl.when(jnp.logical_not(stays(h, other)))
          def _():
              spread(h, other, False).wait_send()


def learn_and_decode(context, out_grad, rewards, counts, heads, master, first_moment, second_moment):
    dma = pltpu.SemaphoreType.DMA
    vmem = pltpu.VMEM
    tokens, width = context.shape
    grid_all = [pl.BlockSpec(memory_space=pl.ANY)] * 2 + [pl.BlockSpec(memory_space=pltpu.SMEM)]
    grid_all += [pl.BlockSpec(memory_space=pltpu.VMEM)] * 5
    return pl.pallas_call(
        step_kernel,
        out_shape=(
            jax.ShapeDtypeStruct((ROWS, width), F32),
            jax.ShapeDtypeStruct((LANE, 8 * width), BF),
        ),
        in_specs=grid_all,
        out_specs=(pl.BlockSpec(memory_space=pltpu.VMEM), pl.BlockSpec(memory_space=pltpu.VMEM)),
        scratch_shapes=[
            vmem((4, CHUNKS, tokens, LANE), BF),
            vmem((2, CHUNKS, tokens, LANE), BF),
            vmem((2, tokens, width), BF),
            vmem((16, 8, LANE), F32),
            vmem((8, LANE), F32),
            vmem((12, LANE, width), F32),
            vmem((CHUNKS, 4, LANE, width), BF),
            vmem((CHUNKS, 4, LANE, width), BF),
            vmem((CHUNKS, 4, LANE, width), BF),
            vmem((CHUNKS, 3, LANE, width), BF),
            vmem((CHUNKS, LANE, width), BF),
            vmem((2, ROWS, width), BF),
            vmem((4, width, LANE), BF),
            vmem((4, width, LANE), BF),
            vmem((4, 4, ROWS, LANE), BF),
            vmem((16, LANE, ROWS), BF),
            vmem((ROWS, width), BF),
            vmem((4, 2, CHUNKS, LANE, LANE), BF),
            vmem((4, 2, CHUNKS, LANE, LANE), BF),
            vmem((4, 2, CHUNKS, LANE, LANE), BF),
            vmem((3, 2, CHUNKS, LANE, LANE), BF),
            vmem((CHUNKS, LANE, LANE), F32),
            vmem((CHUNKS, LANE, LANE), BF),
            vmem((CHUNKS, LANE, LANE), BF),
            vmem((8, CHUNKS, LANE, LANE), BF),
            dma((2, CHUNKS)),
            dma((2, CHUNKS)), dma((2, CHUNKS)),
            dma((2, CHUNKS)), dma((2, CHUNKS)),
            dma((CHUNKS,)), dma((CHUNKS,)),
            dma((16,)), dma((16,)),
            dma((CHUNKS, 4)), dma((CHUNKS, 4)),
            dma((CHUNKS, 3)), dma((CHUNKS, 3)),
            dma((CHUNKS, 2)), dma((2, 3)),
            dma((4,)), dma((4,)),
            dma((4,)), dma((4,)),
            dma((2, 2)), dma((4,)),
            dma((2, 4)), dma((2, 4)),
            dma((2, 3)), dma((2, 3)),
            dma((2,)), dma((2,)),
            dma((2, 7)), dma((2, 8)),
        ],
        compiler_params=pltpu.CompilerParams(
            collective_id=0, has_side_effects=True, vmem_limit_bytes=62 * 1024 * 1024
        ),
        cost_estimate=pl.CostEstimate(flops=14_300_000_000, bytes_accessed=10_000_000, transcendentals=0),
        name="learn_and_decode",
    )(context, out_grad, rewards, counts, heads, master, first_moment, second_moment)


def rotate(vectors, positions):
    half_dim = vectors.shape[-1] // 2
    frequency = rope_base ** (-2.0 * jnp.arange(half_dim, dtype=jnp.float32) / vectors.shape[-1])
    angles = positions[..., None].astype(jnp.float32) * frequency
    cosine_table = jnp.cos(angles)
    sine_table = jnp.sin(angles)
    former = vectors[..., :half_dim]
    latter = vectors[..., half_dim:]
    return jnp.concatenate(
        [former * cosine_table - latter * sine_table, latter * cosine_table + former * sine_table],
        axis=-1,
    )


def attend(queries, old_keys, old_values, new_keys, new_values, live_mask):
    score_scale = HEAD_DIM ** (-0.5)
    step_total = queries.shape[0]
    cache_scores = (
        jnp.einsum("tsgqd,scgd->tsgqc", queries, old_keys, preferred_element_type=jnp.float32)
        * score_scale
    )
    cache_scores = jnp.where(live_mask[None, :, None, None, :], cache_scores, -1e30)
    recent = (
        jnp.einsum("tsgqd,usgd->tsgqu", queries, new_keys, preferred_element_type=jnp.float32)
        * score_scale
    )
    causal = jnp.arange(step_total)[:, None] >= jnp.arange(step_total)[None, :]
    recent = jnp.where(causal[:, None, None, None, :], recent, -1e30)
    row_peak = jnp.maximum(jnp.max(cache_scores, axis=-1), jnp.max(recent, axis=-1))[..., None]
    cache_exp = jnp.exp(cache_scores - row_peak)
    recent_exp = jnp.exp(recent - row_peak)
    denominator = jnp.sum(cache_exp, axis=-1, keepdims=True) + jnp.sum(
        recent_exp, axis=-1, keepdims=True
    )
    cache_weight = (cache_exp / denominator).astype(jnp.bfloat16)
    recent_weight = (recent_exp / denominator).astype(jnp.bfloat16)
    attended = jnp.einsum(
        "tsgqc,scgd->tsgqd", cache_weight, old_values, preferred_element_type=jnp.float32
    )
    attended = attended + jnp.einsum(
        "tsgqu,usgd->tsgqd", recent_weight, new_values, preferred_element_type=jnp.float32
    )
    return attended.astype(jnp.bfloat16)


def per_device(
    context,
    out_grad,
    rewards,
    master,
    first_moment,
    second_moment,
    inputs,
    w_query,
    w_key,
    w_value,
    cache_keys,
    cache_values,
    lengths,
):
    counts = jnp.broadcast_to(
        jnp.sum(rewards, axis=1).astype(F32)[:, None], (rewards.shape[0], LANE)
    )
    step_total, seq_local, model_width = inputs.shape
    local_heads = w_query.shape[1] // HEAD_DIM
    local_kv = w_key.shape[1] // HEAD_DIM
    flat_rows = inputs.reshape(step_total * seq_local, model_width)
    projected = lax.optimization_barrier(jnp.dot(flat_rows, w_query, preferred_element_type=F32))
    queries = projected.reshape(step_total, seq_local, local_heads, HEAD_DIM)
    key_new = jnp.dot(flat_rows, w_key, preferred_element_type=F32).reshape(
        step_total, seq_local, local_kv, HEAD_DIM
    )
    value_new = (
        jnp.dot(flat_rows, w_value, preferred_element_type=F32)
        .reshape(step_total, seq_local, local_kv, HEAD_DIM)
        .astype(BF)
    )
    seq_length = jnp.repeat(lengths, seq_local // lengths.shape[0])
    positions = seq_length[None, :] + jnp.arange(step_total, dtype=jnp.int32)[:, None]
    queries = rotate(queries, positions[:, :, None]).astype(BF)
    queries = queries.reshape(step_total, seq_local, local_kv, local_heads // local_kv, HEAD_DIM)
    key_new = rotate(key_new, positions[:, :, None]).astype(BF)
    slot_total = cache_keys.shape[1]
    old_keys = cache_keys.reshape(seq_local, slot_total, local_kv, HEAD_DIM)
    old_values = cache_values.reshape(seq_local, slot_total, local_kv, HEAD_DIM)
    live_mask = jnp.arange(slot_total, dtype=jnp.int32)[None, :] < seq_length[:, None]
    attended = attend(queries, old_keys, old_values, key_new, value_new, live_mask)
    heads = attended.reshape(step_total * seq_local, local_heads * HEAD_DIM).T
    adam_step, decoded = learn_and_decode(
        context, out_grad, rewards, counts, heads, master, first_moment, second_moment
    )
    return (decoded.reshape(step_total, seq_local, model_width), adam_step)


def solution(mesh):
    placed = (
        P("rep", "tp"),
        P("rep", "tp"),
        P(None, "rep"),
        P("rep", "tp"),
        P("rep", "tp"),
        P("rep", "tp"),
        P(None, "rep", None),
        P(None, "tp"),
        P(None, "tp"),
        P(None, "tp"),
        P("rep", None, "tp"),
        P("rep", None, "tp"),
        P("rep"),
    )
    return jax.shard_map(
        per_device,
        mesh=mesh,
        in_specs=placed,
        out_specs=(P(None, "rep", None), P("rep", "tp")),
        check_vma=False,
    )
```

```python
import jax
import jax.numpy as jnp
from jax import lax
from jax.experimental import pallas as pl
from jax.experimental.pallas import tpu as pltpu
from jax.sharding import PartitionSpec as P

HEAD_DIM = 128

rope_base = 1000000.0
first_beta = 0.9
second_beta = 0.95
adam_epsilon = 1e-08
step_count = 10
learn_rate = 0.001

MESH = pl.DeviceIdType.MESH
LANE = 128
CHUNKS = 5
HALF = 1024
SPANS = ((0, 3), (3, 2))
ROWS = 320
CACHE = 256
BF, F32 = jnp.bfloat16, jnp.float32


def device(x, yl, c, z, yh):
    return {"rep": (x * 2 + yl) * 2 + c, "tp": z * 2 + yh}


def step_kernel(
    ctx, outg, rewards, lengths, cosine, sine, tokens_in, w_query, w_query_rows, w_key, w_value,
    old_keys, old_values, master_in, first_in, second_in,
    adam, decoded,
    cb, sr, ss, tot, totf, keep, give, got, part, xb, tb, ob,
    ag, hx, ab, aa, wb, dgive, dgot, dpart, dxb, dkeep, dys, dyb, dec,
    load_sem, c_send, c_recv, f_send, f_recv, s_send, s_recv,
    t_send, t_recv, d_send, d_recv, x_send, x_recv, o_send, o_recv,
    g_send, g_recv, i_send, i_recv, a_send, a_recv,
    e_send, e_recv, h_send, h_recv, y_send, y_recv, l_send, l_recv,
    xs, qa, ka, va, qb, kn, vn, kf, vf, att, hb, master, first_m, second_m,
    w_sem, k_sem, m_sem,
):
    rep = lax.axis_index("rep")
    tp = lax.axis_index("tp")
    x, yl, c, z, yh = rep // 4, (rep // 2) % 2, rep % 2, tp // 2, tp % 2
    z_up = device(x, yl, c, (z + 1) % 4, yh)
    z_dn = device(x, yl, c, (z + 3) % 4, yh)
    across = device(x, yl, c, z, 1 - yh)
    mate = device(x, yl, 1 - c, z, yh)
    beside = device(x, 1 - yl, c, z, yh)

    def load(src, dst, j, k):
        return pltpu.make_async_copy(src.at[:, pl.ds(j * LANE, LANE)], dst, load_sem.at[k, j])

    for j in range(CHUNKS):
        load(ctx, cb.at[0, j], j, 0).start()
        load(outg, sr.at[0, j], j, 1).start()

    weight_loads = (
        pltpu.make_async_copy(w_query.at[pl.ds(0, 3)], give.at[pl.ds(2, 3)], w_sem.at[0]),
        pltpu.make_async_copy(w_query.at[pl.ds(3, 3)], part.at[pl.ds(2, 3)], w_sem.at[1]),
        pltpu.make_async_copy(w_query_rows.at[pl.ds(3072, 2048)], ss.at[1], w_sem.at[4]),
        pltpu.make_async_copy(w_key, dgive, w_sem.at[2]),
        pltpu.make_async_copy(w_value, dpart, w_sem.at[3]),
    )

    def cache_loads(g):
        seqs = pl.ds(g * 8, 8)
        return (
            pltpu.make_async_copy(old_keys.at[seqs], kf.at[g, :, pl.ds(0, CACHE)], k_sem.at[g, 0]),
            pltpu.make_async_copy(old_values.at[seqs], vf.at[g, :, pl.ds(0, CACHE)], k_sem.at[g, 1]),
        )

    late_loads = (
        pltpu.make_async_copy(master_in, master, m_sem.at[0]),
        pltpu.make_async_copy(first_in, first_m, m_sem.at[1]),
        pltpu.make_async_copy(second_in, second_m, m_sem.at[2]),
    )
    token_load = pltpu.make_async_copy(tokens_in, xs, m_sem.at[3])
    token_load.start()
    for copy in weight_loads:
        copy.start()
    for g in range(4):
        for copy in cache_loads(g):
            copy.start()

    barrier = pltpu.get_barrier_semaphore()

    def greet(target):
        pl.semaphore_signal(barrier, inc=1, device_id=target, device_id_type=MESH)

    @pl.loop(1, 32)
    def _(d):
        e = (rep * 2 + yh + d) % 32
        greet({"rep": e // 2, "tp": z * 2 + e % 2})

    @pl.loop(0, 6)
    def _(d):
        greet({"rep": rep, "tp": (z * 2 + 2 + d) % 8})

    pl.semaphore_wait(barrier, 37)

    def send(src, dst, ss_, rs_, target):
        return pltpu.make_async_remote_copy(
            src_ref=src, dst_ref=dst, send_sem=ss_, recv_sem=rs_,
            device_id=target, device_id_type=MESH,
        )

    first, second = pl.ds(0, HALF), pl.ds(HALF, HALF)

    def own_up(j):
        return send(cb.at[0, j], cb.at[1, j], c_send.at[0, j], c_recv.at[0, j], z_up)

    def own_dn(j):
        return send(cb.at[0, j], cb.at[3, j], c_send.at[1, j], c_recv.at[1, j], z_dn)

    def fwd_up(j):
        return send(cb.at[1, j, first], cb.at[2, j, first], f_send.at[0, j], f_recv.at[0, j], z_up)

    def fwd_dn(j):
        return send(cb.at[3, j, second], cb.at[2, j, second], f_send.at[1, j], f_recv.at[1, j], z_dn)

    def trade(j):
        return send(sr.at[0, j], sr.at[1, j], s_send.at[j], s_recv.at[j], across)

    def heads_z(dz):
        return send(ag.at[0], ag.at[dz], g_send.at[dz], g_recv.at[dz], device(x, yl, c, (z + dz) % 4, yh))


    for j in range(CHUNKS):
        load(ctx, cb.at[0, j], j, 0).wait()
        if j < 2:
            own_up(j).start()
            own_dn(j).start()
        load(outg, sr.at[0, j], j, 1).wait()
        if j < 1: trade(j).start()

    for p in range(8):
        count = rewards[p, 0] + rewards[p, 1] + rewards[p, 2] + rewards[p, 3]
        tot[0, p : p + 1, :] = jnp.full((1, LANE), count.astype(F32))

    def count_copy(d):
        return send(tot.at[0], tot.at[d], t_send.at[d], t_recv.at[d], {"rep": (rep + d) % 16, "tp": tp})

    @pl.loop(1, 16)
    def _(d):
        count_copy(d).start()

    @pl.loop(1, 16)
    def _(d):
        count_copy(d).wait()

    totf[...] = jnp.sum(tot[...], axis=0) * (1.0 / 64.0)

    def scale(rel):
        @pl.loop(0, 32)
        def _(seg):
            rows = pl.ds(pl.multiple_of(seg * 64, 64), 64)
            p = seg // 4
            factor = (rewards[p, seg % 4].astype(F32) - totf[pl.ds(p, 1), :]) * (1.0 / 32768.0)
            for j in range(CHUNKS):
                ss[rel, rows, j * LANE : (j + 1) * LANE] = (
                    sr[rel, j, rows, :].astype(F32) * factor
                ).astype(BF)

    scale(0)
    for copy in late_loads:
        copy.start()

    def attention():
        qa[...] = jnp.zeros_like(qa)
        ka[...] = jnp.zeros_like(ka)
        va[...] = jnp.zeros_like(va)
        token_load.wait()
        for copy in weight_loads:
            copy.wait()

        @pl.loop(0, 3)
        def _(n):
            for base, held in ((0, give), (1536, part)):
                some = xs[:, pl.ds(pl.multiple_of(base + n * 512, 512), 512)]
                qa[...] += jnp.dot(some, held[n + 2].reshape(512, 640), preferred_element_type=F32)

        @pl.loop(0, 4)
        def _(n):
            some = xs[:, pl.ds(pl.multiple_of(3072 + n * 512, 512), 512)]
            held = ss[1, pl.ds(pl.multiple_of(n * 512, 512), 512), :]
            qa[...] += jnp.dot(some, held, preferred_element_type=F32)

        @pl.loop(0, 8)
        def _(m):
            some = xs[:, pl.ds(pl.multiple_of(m * 640, 640), 640)]
            ka[...] += jnp.dot(some, dgive[m // 2, m % 2].reshape(640, LANE), preferred_element_type=F32)
            va[...] += jnp.dot(some, dpart[m // 2, m % 2].reshape(640, LANE), preferred_element_type=F32)

    def attention_scores():
        qb[...] = jnp.zeros_like(qb)
        kn[...] = jnp.zeros_like(kn)
        vn[...] = jnp.zeros_like(vn)

        def turned(vectors):
            return vectors * cosine[...] + pltpu.roll(vectors, 64, 1) * sine[...]

        def rounded(vectors):
            return vectors.astype(BF).astype(F32)

        for h in range(5):
            turned_query = rounded(turned(qa[:, h * LANE : (h + 1) * LANE]))
            for t in range(4):
                qb[:, t * 5 + h, :] = turned_query[t * 32 : (t + 1) * 32]
        turned_key = rounded(turned(ka[...]))
        value = rounded(va[...])
        for t in range(4):
            kn[:, t, :] = turned_key[t * 32 : (t + 1) * 32]
            vn[:, t, :] = value[t * 32 : (t + 1) * 32]

        column = lax.broadcasted_iota(jnp.int32, (24, CACHE + 16), 1)
        row = lax.broadcasted_iota(jnp.int32, (24, CACHE + 16), 0)
        fresh = jnp.logical_and(
            jnp.logical_and(column >= CACHE, column < CACHE + 4), (column - CACHE) * 5 <= row
        )

        @pl.loop(0, 4)
        def _(g):
            slot = g
            for copy in cache_loads(g):
                copy.wait()
            live = jnp.logical_or(column < lengths[g], fresh)

            @pl.loop(0, 8)
            def _(i):
                s = g * 8 + i
                kf[slot, i, CACHE : CACHE + 16, :] = kn[s].astype(BF)
                vf[slot, i, CACHE : CACHE + 16, :] = vn[s].astype(BF)
                scores = lax.dot_general(
                    qb[s].astype(BF), kf[slot, i], (((1,), (1,)), ((), ())), preferred_element_type=F32
                ) * (HEAD_DIM**-0.5)
                scores = jnp.where(live, scores, -1e30)
                grown = jnp.exp(scores - jnp.max(scores, axis=-1, keepdims=True))
                weights = (grown / jnp.sum(grown, axis=-1, keepdims=True)).astype(BF)
                att[s] = jnp.dot(weights, vf[slot, i], preferred_element_type=F32)

        for h in range(5):
            for t in range(4):
                hb[t * 32 : (t + 1) * 32, :] = att[:, t * 5 + h, :]
            ag[0, h * LANE : (h + 1) * LANE, :] = hb[...].T.astype(BF)

    def step(j):
        own_up(j).wait_recv()
        fwd_up(j).start()
        own_dn(j).wait_recv()
        fwd_dn(j).start()
        if j + 2 < CHUNKS:
            own_up(j + 2).start()
            own_dn(j + 2).start()

    def far(j):
        fwd_up(j).wait_recv()
        fwd_dn(j).wait_recv()

    def hand(j, r):
        return send(give.at[j, r], got.at[j, r], d_send.at[j, r], d_recv.at[j, r], mate)

    def over_x(j, r, dx):
        slot = (dx + 3) % 4
        return send(part.at[j, r], xb.at[j, slot], x_send.at[j, slot], x_recv.at[j, slot],
                    device((x + dx) % 4, yl, c, z, yh))

    def contribute(low, high, rels):
        count = (high - low) * len(rels)

        def task(n):
            i = low + n // len(rels)
            rel = rels[0] + n % len(rels)
            rr = i % 4
            return i // 4, rr ^ (rr // 2), rel, (yh + rel) % 2 == c

        def compute(n):
            j, r, rel, mine = task(n)
            block = lax.dot_general(
                cb[r, j], ss[rel], (((0,), (0,)), ((), ())), preferred_element_type=F32
            )

            @pl.when(mine)
            def _():
                keep[n // len(rels)] = block

            @pl.when(jnp.logical_not(mine))
            def _():
                give[j, r] = block.astype(BF)
                hand(j, r).start()

        def pair(n):
            j, r, rel, mine = task(n)

            @pl.when(mine)
            def _():
                hand(j, r).wait_recv()
                part[j, r] = (keep[n // len(rels)] + got[j, r].astype(F32)).astype(BF)
                dx = (z - r - x + 8) % 4

                @pl.when(dx != 0)
                def _():
                    over_x(j, r, dx).start()

        @pl.loop(0, count + 2)
        def _(n):
            @pl.when(n < count)
            def _():
                compute(n)

            @pl.when(n >= 2)
            def _():
                pair(n - 2)

    def pieces(j):
        if j < 2:
            return ((0, 128, 0, 128 * j, j),)
        if j > 2:
            return ((0, 128, 1, 128 * j - ROWS, j - 2),)
        return ((0, 64, 0, 256, 2), (64, 64, 1, 0, 0))

    def to_owner(j, piece, local):
        at, rows, core, row, k = piece
        src = tb.at[j, pl.ds(at, rows)]
        dst = ob.at[yl, pl.ds(row, rows)]
        if local:
            return pltpu.make_async_copy(src, dst, o_recv.at[yl, k])
        return send(src, dst, o_send.at[j, at // 64], o_recv.at[yl, k], device(x, yh, core, z, c))

    def is_me(core):
        return jnp.logical_and(jnp.logical_and(c == yh, yh == yl), c == core)

    def x_sum(j):
        total = part[j, (z - x + 4) % 4].astype(F32)
        for slot in range(3):
            over_x(j, 0, slot + 1).wait_recv()
            total = total + xb[j, slot].astype(F32)
        tb[j] = total.astype(BF)
        for piece in pieces(j):
            @pl.when(is_me(piece[2]))
            def _():
                to_owner(j, piece, True).start()

            @pl.when(jnp.logical_not(is_me(piece[2])))
            def _():
                to_owner(j, piece, False).start()

    def heads_x(dz, local):
        to = (z - dz + 4) % 4
        if local:
            return pltpu.make_async_copy(ag.at[dz], hx.at[x], i_recv.at[x])
        return send(ag.at[dz], hx.at[x], i_send.at[dz], i_recv.at[x], device(to, yl, c, z, yh))

    def stays_x(dz):
        return (z - dz + 4) % 4 == x

    def heads_over_x():
        for dz in (1, 2, 3):
            heads_z(dz).wait_recv()

        @pl.loop(0, 4)
        def _(dz):
            @pl.when(stays_x(dz))
            def _():
                heads_x(dz, True).start()

            @pl.when(jnp.logical_not(stays_x(dz)))
            def _():
                heads_x(dz, False).start()

    def spread(h, other, local):
        src = hx.at[:, pl.ds(h * ROWS, ROWS)]
        dst = ab.at[yl * 2 + c]
        if local:
            return pltpu.make_async_copy(src, dst, a_recv.at[yl * 2 + c])
        return send(src, dst, a_send.at[h, other], a_recv.at[yl * 2 + c], device(x, yh, h, z, other))

    def stays(h, other):
        return jnp.logical_and(yh == yl, jnp.logical_and(h == c, other == yh))

    def spread_heads():

        @pl.loop(0, 4)
        def _(k):
            pltpu.make_async_copy(hx.at[k], hx.at[k], i_recv.at[k]).wait()

    def spread_one(h, other):
        @pl.when(stays(h, other))
        def _():
            spread(h, other, True).start()

        @pl.when(jnp.logical_not(stays(h, other)))
        def _():
            spread(h, other, False).start()

    def take_heads():
        for k in range(4):
            pltpu.make_async_copy(ab.at[k], ab.at[k], a_recv.at[k]).wait()

        @pl.loop(0, 16)
        def _(g):
            aa[g] = ab[g // 4, g % 4].T

    step(0)
    trade(1).start()
    contribute(0, 3, (0,))
    step(1)
    trade(2).start()
    contribute(4, 7, (0,))
    attention()
    far(0)
    trade(3).start()
    contribute(3, 4, (0,))
    attention_scores()

    @pl.loop(1, 4)
    def _(dz):
        heads_z(dz).start()

    step(2)
    trade(4).start()
    contribute(8, 11, (0,))
    far(1)
    contribute(7, 8, (0,))
    step(3)
    contribute(12, 15, (0,))
    for j in range(CHUNKS):
        trade(j).wait_recv()
    scale(1)
    contribute(0, 11, (1,))
    heads_over_x()
    far(2)
    contribute(11, 12, (0, 1))
    contribute(12, 15, (1,))
    step(4)
    spread_heads()
    spread_one(0, 0)
    spread_one(0, 1)
    contribute(16, 19, (0, 1))
    spread_one(1, 0)
    spread_one(1, 1)
    x_sum(0)
    x_sum(1)
    far(3)
    contribute(15, 16, (0, 1))
    x_sum(2)
    far(4)
    contribute(19, 20, (0, 1))
    x_sum(3)
    x_sum(4)
    take_heads()

    for core, sizes, starts in ((0, (128, 128, 64), (0, 128, 256)), (1, (64, 128, 128), (0, 64, 192))):
        @pl.when(c == core)
        def _():
            for src in range(2):
                for k in range(3):
                    there = ob.at[src, pl.ds(starts[k], sizes[k])]
                    pltpu.make_async_copy(there, there, o_recv.at[src, k]).wait()

    for copy in late_loads:
        copy.wait()

    @pl.loop(0, ROWS // 32)
    def _(n):
        rows = pl.ds(pl.multiple_of(n * 32, 32), 32)
        gradient = ob[0, rows, :].astype(F32) + ob[1, rows, :].astype(F32)
        moment_new = first_beta * first_m[rows, :] + (1.0 - first_beta) * gradient
        square_new = second_beta * second_m[rows, :] + (1.0 - second_beta) * gradient * gradient
        direction = (
            moment_new
            / (1.0 - first_beta**step_count)
            / (jnp.sqrt(square_new / (1.0 - second_beta**step_count)) + adam_epsilon)
        )
        adam[rows, :] = direction
        wb[rows, :] = (master[rows, :] - learn_rate * direction).astype(BF)

    def blocks(q):
        return pl.ds(*SPANS[q])

    def d_hand(q, xg):
        return send(dgive.at[xg, :, blocks(q)], dgot.at[xg, :, blocks(q)], e_send.at[q, xg], e_recv.at[q, xg], mate)

    def d_over_x(q, dx):
        slot = (dx + 3) % 4
        to = (x + dx) % 4
        return send(dpart.at[to, :, blocks(q)], dxb.at[slot, :, blocks(q)], h_send.at[q, slot], h_recv.at[q, slot],
                    device(to, yl, c, z, yh))

    def d_beside(q):
        return send(dys.at[blocks(q)], dyb.at[blocks(q)], y_send.at[q], y_recv.at[q], beside)

    def d_across(q):
        there = dec.at[tp, blocks(q)]
        return send(there, there, l_send.at[q, 0], l_recv.at[q, tp], across)

    def d_over_z(q, dz, other):
        mine = z * 2 + (1 - yh if other else yh)
        there = dec.at[mine, blocks(q)]
        return send(there, there, l_send.at[q, dz + 3 * other], l_recv.at[q, mine],
                    device(x, yl, c, (z + dz) % 4, yh))

    def d_multiply(q):
        start, width = SPANS[q]
        columns = slice(start * LANE, (start + width) * LANE)

        @pl.loop(0, 8)
        def _(n):
            xg, side = (x + n // 2 + 2) % 4, n % 2
            block = jnp.dot(aa[side * 8 + (1 - c) * 4 + xg], wb[:, columns], preferred_element_type=F32)
            for b in range(width):
                dgive[xg, side, start + b] = block[:, b * LANE : (b + 1) * LANE].astype(BF)

            @pl.when(side == 1)
            def _():
                d_hand(q, xg).start()

        @pl.loop(0, 8)
        def _(n):
            dx, side = (n // 2 + 2) % 4, n % 2
            xg = (x + dx) % 4
            block = jnp.dot(aa[side * 8 + c * 4 + xg], wb[:, columns], preferred_element_type=F32)

            @pl.when(side == 0)
            def _():
                d_hand(q, xg).wait_recv()

            for b in range(width):
                dpart[xg, side, start + b] = (
                    block[:, b * LANE : (b + 1) * LANE] + dgot[xg, side, start + b].astype(F32)
                ).astype(BF)

            if q == 0:
                @pl.when(jnp.logical_and(side == 1, dx != 0))
                def _():
                    d_over_x(q, dx).start()

    def d_x_sum(q):
        start, width = SPANS[q]
        for dx in (1, 3, 2):
            d_over_x(q, dx).wait_recv()

        def total(side, b):
            value = dpart[x, side, b].astype(F32)
            for slot in range(3):
                value = value + dxb[slot, side, b].astype(F32)
            return value

        for b in range(start, start + width):
            dys[b] = total(1 - yl, b).astype(BF)
        d_beside(q).start()
        for b in range(start, start + width):
            dkeep[b] = total(yl, b)

    def d_finish(q):
        start, width = SPANS[q]
        d_beside(q).wait_recv()
        for b in range(start, start + width):
            dec[tp, b] = (dkeep[b] + dyb[b].astype(F32)).astype(BF)
        for dz in (2, 1, 3):
            d_over_z(q, dz, 0).start()
        d_across(q).start()

    def d_pass(q):
        other = dec.at[z * 2 + 1 - yh, blocks(q)]
        pltpu.make_async_copy(other, other, l_recv.at[q, z * 2 + 1 - yh]).wait()
        for dz in (2, 1, 3):
            d_over_z(q, dz, 1).start()

    d_multiply(0)
    if len(SPANS) > 1:
        d_multiply(1)
    d_x_sum(0)
    if len(SPANS) > 1:
        for dx in (2, 1, 3):
            d_over_x(1, dx).start()
    d_finish(0)
    d_pass(0)
    if len(SPANS) > 1:
        d_x_sum(1)
        d_finish(1)
        d_pass(1)

    for q in range(len(SPANS)):
        start, width = SPANS[q]

        @pl.loop(2, 8)
        def _(d):
            t = (z * 2 + d) % 8
            pltpu.make_async_copy(dec.at[t, blocks(q)], dec.at[t, blocks(q)], l_recv.at[q, t]).wait()

        for t in range(8):
            for b in range(start, start + width):
                decoded[:, t * 640 + b * LANE : t * 640 + (b + 1) * LANE] = dec[t, b]

    for j in range(CHUNKS):
        for copy in (own_up(j), own_dn(j), fwd_up(j), fwd_dn(j)) + (trade(j),):
            copy.wait_send()

        @pl.loop(0, 4)
        def _(r):
          hand(j, r).wait_send()

        if j < len(SPANS):
          @pl.loop(0, 4)
          def _(k):
            d_hand(j, k).wait_send()

          d_beside(j).wait_send()
          d_across(j).wait_send()
          for dz in (1, 2, 3):
            d_over_x(j, dz).wait_send()
            d_over_z(j, dz, 0).wait_send()
            d_over_z(j, dz, 1).wait_send()

        for dx in (1, 2, 3):
            over_x(j, 0, dx).wait_send()
        for piece in pieces(j):
          @pl.when(jnp.logical_not(is_me(piece[2])))
          def _():
              to_owner(j, piece, False).wait_send()

    for dz in (1, 2, 3):
      heads_z(dz).wait_send()

    @pl.loop(0, 4)
    def _(dz):
      @pl.when(jnp.logical_not(stays_x(dz)))
      def _():
          heads_x(dz, False).wait_send()

    for h in range(2):
      for other in range(2):
          @pl.when(jnp.logical_not(stays(h, other)))
          def _():
              spread(h, other, False).wait_send()


def learn_and_decode(
    context, out_grad, rewards, lengths, cosine, sine, tokens_in, w_query, w_query_rows, w_key, w_value,
    old_keys, old_values, master, first_moment, second_moment,
):
    dma = pltpu.SemaphoreType.DMA
    vmem = pltpu.VMEM
    tokens, width = context.shape
    anywhere = pl.BlockSpec(memory_space=pl.ANY)
    in_smem = pl.BlockSpec(memory_space=pltpu.SMEM)
    in_vmem = pl.BlockSpec(memory_space=pltpu.VMEM)
    grid_all = [anywhere] * 2 + [in_smem] * 2 + [in_vmem] * 2 + [anywhere] * 10
    return pl.pallas_call(
        step_kernel,
        out_shape=(
            jax.ShapeDtypeStruct((ROWS, width), F32),
            jax.ShapeDtypeStruct((LANE, 8 * width), BF),
        ),
        in_specs=grid_all,
        out_specs=(pl.BlockSpec(memory_space=pltpu.VMEM), pl.BlockSpec(memory_space=pltpu.VMEM)),
        scratch_shapes=[
            vmem((4, CHUNKS, tokens, LANE), BF),
            vmem((2, CHUNKS, tokens, LANE), BF),
            vmem((2, tokens, width), BF),
            vmem((16, 8, LANE), F32),
            vmem((8, LANE), F32),
            vmem((12, LANE, width), F32),
            vmem((CHUNKS, 4, LANE, width), BF),
            vmem((CHUNKS, 4, LANE, width), BF),
            vmem((CHUNKS, 4, LANE, width), BF),
            vmem((CHUNKS, 3, LANE, width), BF),
            vmem((CHUNKS, LANE, width), BF),
            vmem((2, ROWS, width), BF),
            vmem((4, width, LANE), BF),
            vmem((4, width, LANE), BF),
            vmem((4, 4, ROWS, LANE), BF),
            vmem((16, LANE, ROWS), BF),
            vmem((ROWS, width), BF),
            vmem((4, 2, CHUNKS, LANE, LANE), BF),
            vmem((4, 2, CHUNKS, LANE, LANE), BF),
            vmem((4, 2, CHUNKS, LANE, LANE), BF),
            vmem((3, 2, CHUNKS, LANE, LANE), BF),
            vmem((CHUNKS, LANE, LANE), F32),
            vmem((CHUNKS, LANE, LANE), BF),
            vmem((CHUNKS, LANE, LANE), BF),
            vmem((8, CHUNKS, LANE, LANE), BF),
            dma((2, CHUNKS)),
            dma((2, CHUNKS)), dma((2, CHUNKS)),
            dma((2, CHUNKS)), dma((2, CHUNKS)),
            dma((CHUNKS,)), dma((CHUNKS,)),
            dma((16,)), dma((16,)),
            dma((CHUNKS, 4)), dma((CHUNKS, 4)),
            dma((CHUNKS, 3)), dma((CHUNKS, 3)),
            dma((CHUNKS, 2)), dma((2, 3)),
            dma((4,)), dma((4,)),
            dma((4,)), dma((4,)),
            dma((2, 2)), dma((4,)),
            dma((2, 4)), dma((2, 4)),
            dma((2, 3)), dma((2, 3)),
            dma((2,)), dma((2,)),
            dma((2, 7)), dma((2, 8)),
            vmem((LANE, 8 * width), BF),
            vmem((LANE, width), F32), vmem((LANE, LANE), F32), vmem((LANE, LANE), F32),
            vmem((32, 24, LANE), F32), vmem((32, 16, LANE), F32), vmem((32, 16, LANE), F32),
            vmem((4, 8, CACHE + 16, LANE), BF), vmem((4, 8, CACHE + 16, LANE), BF),
            vmem((32, 24, LANE), F32), vmem((LANE, LANE), F32),
            vmem((ROWS, width), F32), vmem((ROWS, width), F32), vmem((ROWS, width), F32),
            dma((5,)), dma((4, 2)), dma((4,)),
        ],
        compiler_params=pltpu.CompilerParams(
            collective_id=0, has_side_effects=True, vmem_limit_bytes=63 * 1024 * 1024
        ),
        cost_estimate=pl.CostEstimate(flops=14_300_000_000, bytes_accessed=10_000_000, transcendentals=0),
        name="learn_and_decode",
    )(
        context, out_grad, rewards, lengths, cosine, sine, tokens_in, w_query, w_query_rows, w_key, w_value,
        old_keys, old_values, master, first_moment, second_moment,
    )


def per_device(
    context,
    out_grad,
    rewards,
    master,
    first_moment,
    second_moment,
    inputs,
    w_query,
    w_key,
    w_value,
    cache_keys,
    cache_values,
    lengths,
):
    step_total, seq_local, model_width = inputs.shape
    seq_length = jnp.repeat(lengths, seq_local // lengths.shape[0])
    positions = seq_length[None, :] + jnp.arange(step_total, dtype=jnp.int32)[:, None]
    half_dim = HEAD_DIM // 2
    frequency = rope_base ** (-2.0 * jnp.arange(half_dim, dtype=F32) / HEAD_DIM)
    angles = positions.reshape(-1, 1).astype(F32) * frequency
    cosine = jnp.concatenate([jnp.cos(angles), jnp.cos(angles)], axis=1)
    sine = jnp.concatenate([-jnp.sin(angles), jnp.sin(angles)], axis=1)
    adam_step, decoded = learn_and_decode(
        context, out_grad, rewards, lengths, cosine, sine,
        inputs.reshape(step_total * seq_local, model_width),
        w_query.reshape(10, 4, LANE, 5 * LANE), w_query,
        w_key.reshape(4, 2, CHUNKS, LANE, LANE), w_value.reshape(4, 2, CHUNKS, LANE, LANE),
        cache_keys, cache_values, master, first_moment, second_moment,
    )
    return (decoded.reshape(step_total, seq_local, model_width), adam_step)


def solution(mesh):
    placed = (
        P("rep", "tp"),
        P("rep", "tp"),
        P(None, "rep"),
        P("rep", "tp"),
        P("rep", "tp"),
        P("rep", "tp"),
        P(None, "rep", None),
        P(None, "tp"),
        P(None, "tp"),
        P(None, "tp"),
        P("rep", None, "tp"),
        P("rep", None, "tp"),
        P("rep"),
    )
    return jax.shard_map(
        per_device,
        mesh=mesh,
        in_specs=placed,
        out_specs=(P(None, "rep", None), P("rep", "tp")),
        check_vma=False,
    )
```

```python
import jax
import jax.numpy as jnp
from jax import lax
from jax.experimental import pallas as pl
from jax.experimental.pallas import tpu as pltpu
from jax.sharding import PartitionSpec as P

HEAD_DIM = 128

rope_base = 1000000.0
first_beta = 0.9
second_beta = 0.95
adam_epsilon = 1e-08
step_count = 10
learn_rate = 0.001

MESH = pl.DeviceIdType.MESH
LANE = 128
CHUNKS = 5
HALF = 1024
SPANS = ((0, 3), (3, 2))
ROWS = 320
CACHE = 256
BF, F32 = jnp.bfloat16, jnp.float32


def device(x, yl, c, z, yh):
    return {"rep": (x * 2 + yl) * 2 + c, "tp": z * 2 + yh}


def step_kernel(
    ctx, outg, rewards, lengths, cosine, sine, tokens_in, w_query, w_query_rows, w_key, w_value,
    old_keys, old_values, master_in, first_in, second_in,
    adam, decoded,
    cb, sr, ss, tot, totf, keep, give, got, part, xb, tb, ob,
    ag, hx, ab, aa, wb, dgive, dgot, dpart, dxb, dkeep, dys, dyb, dec,
    load_sem, c_send, c_recv, f_send, f_recv, s_send, s_recv,
    t_send, t_recv, d_send, d_recv, x_send, x_recv, o_send, o_recv,
    g_send, g_recv, i_send, i_recv, a_send, a_recv,
    e_send, e_recv, h_send, h_recv, y_send, y_recv, l_send, l_recv,
    xs, qa, ka, va, qb, kn, vn, kf, vf, att, hb, master, first_m, second_m,
    w_sem, k_sem, m_sem,
):
    rep = lax.axis_index("rep")
    tp = lax.axis_index("tp")
    x, yl, c, z, yh = rep // 4, (rep // 2) % 2, rep % 2, tp // 2, tp % 2
    z_up = device(x, yl, c, (z + 1) % 4, yh)
    z_dn = device(x, yl, c, (z + 3) % 4, yh)
    across = device(x, yl, c, z, 1 - yh)
    mate = device(x, yl, 1 - c, z, yh)
    beside = device(x, 1 - yl, c, z, yh)

    def load(src, dst, j, k):
        return pltpu.make_async_copy(src.at[:, pl.ds(j * LANE, LANE)], dst, load_sem.at[k, j])

    for j in range(CHUNKS):
        load(ctx, cb.at[0, j], j, 0).start()
        load(outg, sr.at[0, j], j, 1).start()

    weight_loads = (
        pltpu.make_async_copy(w_query.at[pl.ds(0, 3)], give.at[pl.ds(2, 3)], w_sem.at[0]),
        pltpu.make_async_copy(w_query.at[pl.ds(3, 3)], part.at[pl.ds(2, 3)], w_sem.at[1]),
        pltpu.make_async_copy(w_query_rows.at[pl.ds(3072, 2048)], ss.at[1], w_sem.at[4]),
        pltpu.make_async_copy(w_key, dgive, w_sem.at[2]),
        pltpu.make_async_copy(w_value, dpart, w_sem.at[3]),
    )

    def cache_loads(g):
        seqs = pl.ds(g * 8, 8)
        return (
            pltpu.make_async_copy(old_keys.at[seqs], kf.at[g, :, pl.ds(0, CACHE)], k_sem.at[g, 0]),
            pltpu.make_async_copy(old_values.at[seqs], vf.at[g, :, pl.ds(0, CACHE)], k_sem.at[g, 1]),
        )

    late_loads = (
        pltpu.make_async_copy(master_in, master, m_sem.at[0]),
        pltpu.make_async_copy(first_in, first_m, m_sem.at[1]),
        pltpu.make_async_copy(second_in, second_m, m_sem.at[2]),
    )
    token_load = pltpu.make_async_copy(tokens_in, xs, m_sem.at[3])
    token_load.start()
    for copy in weight_loads:
        copy.start()
    for g in range(4):
        for copy in cache_loads(g):
            copy.start()

    barrier = pltpu.get_barrier_semaphore()

    def greet(target):
        pl.semaphore_signal(barrier, inc=1, device_id=target, device_id_type=MESH)

    @pl.loop(1, 32)
    def _(d):
        e = (rep * 2 + yh + d) % 32
        greet({"rep": e // 2, "tp": z * 2 + e % 2})

    @pl.loop(0, 6)
    def _(d):
        greet({"rep": rep, "tp": (z * 2 + 2 + d) % 8})

    pl.semaphore_wait(barrier, 37)

    def send(src, dst, ss_, rs_, target):
        return pltpu.make_async_remote_copy(
            src_ref=src, dst_ref=dst, send_sem=ss_, recv_sem=rs_,
            device_id=target, device_id_type=MESH,
        )

    first, second = pl.ds(0, HALF), pl.ds(HALF, HALF)

    def own_up(j):
        return send(cb.at[0, j], cb.at[1, j], c_send.at[0, j], c_recv.at[0, j], z_up)

    def own_dn(j):
        return send(cb.at[0, j], cb.at[3, j], c_send.at[1, j], c_recv.at[1, j], z_dn)

    def fwd_up(j):
        return send(cb.at[1, j, first], cb.at[2, j, first], f_send.at[0, j], f_recv.at[0, j], z_up)

    def fwd_dn(j):
        return send(cb.at[3, j, second], cb.at[2, j, second], f_send.at[1, j], f_recv.at[1, j], z_dn)

    def trade(j):
        return send(sr.at[0, j], sr.at[1, j], s_send.at[j], s_recv.at[j], across)

    def heads_z(dz):
        return send(ag.at[0], ag.at[dz], g_send.at[dz], g_recv.at[dz], device(x, yl, c, (z + dz) % 4, yh))


    for j in range(CHUNKS):
        load(ctx, cb.at[0, j], j, 0).wait()
        if j < 2:
            own_up(j).start()
            own_dn(j).start()
        load(outg, sr.at[0, j], j, 1).wait()
        if j < 1: trade(j).start()

    for p in range(8):
        count = rewards[p, 0] + rewards[p, 1] + rewards[p, 2] + rewards[p, 3]
        tot[0, p : p + 1, :] = jnp.full((1, LANE), count.astype(F32))

    def count_copy(d):
        return send(tot.at[0], tot.at[d], t_send.at[d], t_recv.at[d], {"rep": (rep + d) % 16, "tp": tp})

    @pl.loop(1, 16)
    def _(d):
        count_copy(d).start()

    @pl.loop(1, 16)
    def _(d):
        count_copy(d).wait()

    totf[...] = jnp.sum(tot[...], axis=0) * (1.0 / 64.0)

    def scale(rel):
        @pl.loop(0, 32)
        def _(seg):
            rows = pl.ds(pl.multiple_of(seg * 64, 64), 64)
            p = seg // 4
            factor = (rewards[p, seg % 4].astype(F32) - totf[pl.ds(p, 1), :]) * (1.0 / 32768.0)
            for j in range(CHUNKS):
                ss[rel, rows, j * LANE : (j + 1) * LANE] = (
                    sr[rel, j, rows, :].astype(F32) * factor
                ).astype(BF)

    scale(0)
    for copy in late_loads:
        copy.start()

    def attention():
        qa[...] = jnp.zeros_like(qa)
        ka[...] = jnp.zeros_like(ka)
        va[...] = jnp.zeros_like(va)
        token_load.wait()
        for copy in weight_loads:
            copy.wait()

        @pl.loop(0, 3)
        def _(n):
            for base, held in ((0, give), (1536, part)):
                some = xs[:, pl.ds(pl.multiple_of(base + n * 512, 512), 512)]
                qa[...] += jnp.dot(some, held[n + 2].reshape(512, 640), preferred_element_type=F32)

        @pl.loop(0, 4)
        def _(n):
            some = xs[:, pl.ds(pl.multiple_of(3072 + n * 512, 512), 512)]
            held = ss[1, pl.ds(pl.multiple_of(n * 512, 512), 512), :]
            qa[...] += jnp.dot(some, held, preferred_element_type=F32)

        @pl.loop(0, 8)
        def _(m):
            some = xs[:, pl.ds(pl.multiple_of(m * 640, 640), 640)]
            ka[...] += jnp.dot(some, dgive[m // 2, m % 2].reshape(640, LANE), preferred_element_type=F32)
            va[...] += jnp.dot(some, dpart[m // 2, m % 2].reshape(640, LANE), preferred_element_type=F32)

    def attention_scores():
        qb[...] = jnp.zeros_like(qb)
        kn[...] = jnp.zeros_like(kn)
        vn[...] = jnp.zeros_like(vn)

        def turned(vectors):
            return vectors * cosine[...] + pltpu.roll(vectors, 64, 1) * sine[...]

        def rounded(vectors):
            return vectors.astype(BF).astype(F32)

        for h in range(5):
            turned_query = rounded(turned(qa[:, h * LANE : (h + 1) * LANE]))
            for t in range(4):
                qb[:, t * 5 + h, :] = turned_query[t * 32 : (t + 1) * 32]
        turned_key = rounded(turned(ka[...]))
        value = rounded(va[...])
        for t in range(4):
            kn[:, t, :] = turned_key[t * 32 : (t + 1) * 32]
            vn[:, t, :] = value[t * 32 : (t + 1) * 32]

        column = lax.broadcasted_iota(jnp.int32, (24, CACHE + 16), 1)
        row = lax.broadcasted_iota(jnp.int32, (24, CACHE + 16), 0)
        fresh = jnp.logical_and(
            jnp.logical_and(column >= CACHE, column < CACHE + 4), (column - CACHE) * 5 <= row
        )

        @pl.loop(0, 4)
        def _(g):
            slot = g
            for copy in cache_loads(g):
                copy.wait()
            live = jnp.logical_or(column < lengths[g], fresh)

            @pl.loop(0, 8)
            def _(i):
                s = g * 8 + i
                kf[slot, i, CACHE : CACHE + 16, :] = kn[s].astype(BF)
                vf[slot, i, CACHE : CACHE + 16, :] = vn[s].astype(BF)
                scores = lax.dot_general(
                    qb[s].astype(BF), kf[slot, i], (((1,), (1,)), ((), ())), preferred_element_type=F32
                ) * (HEAD_DIM**-0.5)
                scores = jnp.where(live, scores, -1e30)
                grown = jnp.exp(scores - jnp.max(scores, axis=-1, keepdims=True))
                weights = (grown / jnp.sum(grown, axis=-1, keepdims=True)).astype(BF)
                att[s] = jnp.dot(weights, vf[slot, i], preferred_element_type=F32)

        for h in range(5):
            for t in range(4):
                hb[t * 32 : (t + 1) * 32, :] = att[:, t * 5 + h, :]
            ag[0, h * LANE : (h + 1) * LANE, :] = hb[...].T.astype(BF)

    def step(j):
        own_up(j).wait_recv()
        fwd_up(j).start()
        own_dn(j).wait_recv()
        fwd_dn(j).start()
        if j + 2 < CHUNKS:
            own_up(j + 2).start()
            own_dn(j + 2).start()

    def far(j):
        fwd_up(j).wait_recv()
        fwd_dn(j).wait_recv()

    def hand(j, r):
        return send(give.at[j, r], got.at[j, r], d_send.at[j, r], d_recv.at[j, r], mate)

    def over_x(j, r, dx):
        slot = (dx + 3) % 4
        return send(part.at[j, r], xb.at[j, slot], x_send.at[j, slot], x_recv.at[j, slot],
                    device((x + dx) % 4, yl, c, z, yh))

    def contribute(low, high, rels):
        count = (high - low) * len(rels)

        def task(n):
            i = low + n // len(rels)
            rel = rels[0] + n % len(rels)
            rr = i % 4
            return i // 4, rr ^ (rr // 2), rel, (yh + rel) % 2 == c

        def compute(n):
            j, r, rel, mine = task(n)
            block = lax.dot_general(
                cb[r, j], ss[rel], (((0,), (0,)), ((), ())), preferred_element_type=F32
            )

            @pl.when(mine)
            def _():
                keep[n // len(rels)] = block

            @pl.when(jnp.logical_not(mine))
            def _():
                give[j, r] = block.astype(BF)
                hand(j, r).start()

        def pair(n):
            j, r, rel, mine = task(n)

            @pl.when(mine)
            def _():
                hand(j, r).wait_recv()
                part[j, r] = (keep[n // len(rels)] + got[j, r].astype(F32)).astype(BF)
                dx = (z - r - x + 8) % 4

                @pl.when(dx != 0)
                def _():
                    over_x(j, r, dx).start()

        @pl.loop(0, count + 2)
        def _(n):
            @pl.when(n < count)
            def _():
                compute(n)

            @pl.when(n >= 2)
            def _():
                pair(n - 2)

    def pieces(j):
        if j < 2:
            return ((0, 128, 0, 128 * j, j),)
        if j > 2:
            return ((0, 128, 1, 128 * j - ROWS, j - 2),)
        return ((0, 64, 0, 256, 2), (64, 64, 1, 0, 0))

    def to_owner(j, piece, local):
        at, rows, core, row, k = piece
        src = tb.at[j, pl.ds(at, rows)]
        dst = ob.at[yl, pl.ds(row, rows)]
        if local:
            return pltpu.make_async_copy(src, dst, o_recv.at[yl, k])
        return send(src, dst, o_send.at[j, at // 64], o_recv.at[yl, k], device(x, yh, core, z, c))

    def is_me(core):
        return jnp.logical_and(jnp.logical_and(c == yh, yh == yl), c == core)

    def x_sum(j):
        total = part[j, (z - x + 4) % 4].astype(F32)
        for slot in range(3):
            over_x(j, 0, slot + 1).wait_recv()
            total = total + xb[j, slot].astype(F32)
        tb[j] = total.astype(BF)
        for piece in pieces(j):
            @pl.when(is_me(piece[2]))
            def _():
                to_owner(j, piece, True).start()

            @pl.when(jnp.logical_not(is_me(piece[2])))
            def _():
                to_owner(j, piece, False).start()

    def heads_x(dz, local):
        to = (z - dz + 4) % 4
        if local:
            return pltpu.make_async_copy(ag.at[dz], hx.at[x], i_recv.at[x])
        return send(ag.at[dz], hx.at[x], i_send.at[dz], i_recv.at[x], device(to, yl, c, z, yh))

    def stays_x(dz):
        return (z - dz + 4) % 4 == x

    def heads_over_x():
        for dz in (1, 2, 3):
            heads_z(dz).wait_recv()

        @pl.loop(0, 4)
        def _(dz):
            @pl.when(stays_x(dz))
            def _():
                heads_x(dz, True).start()

            @pl.when(jnp.logical_not(stays_x(dz)))
            def _():
                heads_x(dz, False).start()

    def spread(h, other, local):
        src = hx.at[:, pl.ds(h * ROWS, ROWS)]
        dst = ab.at[yl * 2 + c]
        if local:
            return pltpu.make_async_copy(src, dst, a_recv.at[yl * 2 + c])
        return send(src, dst, a_send.at[h, other], a_recv.at[yl * 2 + c], device(x, yh, h, z, other))

    def stays(h, other):
        return jnp.logical_and(yh == yl, jnp.logical_and(h == c, other == yh))

    def spread_heads():

        @pl.loop(0, 4)
        def _(k):
            pltpu.make_async_copy(hx.at[k], hx.at[k], i_recv.at[k]).wait()

    def spread_one(h, other):
        @pl.when(stays(h, other))
        def _():
            spread(h, other, True).start()

        @pl.when(jnp.logical_not(stays(h, other)))
        def _():
            spread(h, other, False).start()

    def take_heads():
        for k in range(4):
            pltpu.make_async_copy(ab.at[k], ab.at[k], a_recv.at[k]).wait()

        @pl.loop(0, 16)
        def _(g):
            aa[g] = ab[g // 4, g % 4].T

    step(0)
    trade(1).start()
    contribute(0, 3, (0,))
    step(1)
    trade(2).start()
    contribute(4, 7, (0,))
    attention()
    far(0)
    trade(3).start()
    contribute(3, 4, (0,))
    attention_scores()

    @pl.loop(1, 4)
    def _(dz):
        heads_z(dz).start()

    step(2)
    trade(4).start()
    contribute(8, 11, (0,))
    far(1)
    contribute(7, 8, (0,))
    heads_over_x()
    step(3)
    contribute(12, 15, (0,))
    for j in range(CHUNKS):
        trade(j).wait_recv()
    spread_heads()
    spread_one(0, 0)
    spread_one(0, 1)
    scale(1)
    contribute(0, 11, (1,))
    far(2)
    contribute(11, 12, (0, 1))
    spread_one(1, 0)
    spread_one(1, 1)
    step(4)
    contribute(12, 15, (1,))
    contribute(16, 19, (0, 1))
    x_sum(0)
    far(3)
    contribute(15, 16, (0, 1))
    x_sum(1)
    far(4)
    contribute(19, 20, (0, 1))
    take_heads()
    x_sum(2)
    x_sum(3)
    x_sum(4)

    for core, sizes, starts in ((0, (128, 128, 64), (0, 128, 256)), (1, (64, 128, 128), (0, 64, 192))):
        @pl.when(c == core)
        def _():
            for src in range(2):
                for k in range(3):
                    there = ob.at[src, pl.ds(starts[k], sizes[k])]
                    pltpu.make_async_copy(there, there, o_recv.at[src, k]).wait()

    for copy in late_loads:
        copy.wait()

    @pl.loop(0, ROWS // 32)
    def _(n):
        rows = pl.ds(pl.multiple_of(n * 32, 32), 32)
        gradient = ob[0, rows, :].astype(F32) + ob[1, rows, :].astype(F32)
        moment_new = first_beta * first_m[rows, :] + (1.0 - first_beta) * gradient
        square_new = second_beta * second_m[rows, :] + (1.0 - second_beta) * gradient * gradient
        direction = (
            moment_new
            / (1.0 - first_beta**step_count)
            / (jnp.sqrt(square_new / (1.0 - second_beta**step_count)) + adam_epsilon)
        )
        adam[rows, :] = direction
        wb[rows, :] = (master[rows, :] - learn_rate * direction).astype(BF)

    def blocks(q):
        return pl.ds(*SPANS[q])

    def d_hand(q, xg):
        return send(dgive.at[xg, :, blocks(q)], dgot.at[xg, :, blocks(q)], e_send.at[q, xg], e_recv.at[q, xg], mate)

    def d_over_x(q, dx):
        slot = (dx + 3) % 4
        to = (x + dx) % 4
        return send(dpart.at[to, :, blocks(q)], dxb.at[slot, :, blocks(q)], h_send.at[q, slot], h_recv.at[q, slot],
                    device(to, yl, c, z, yh))

    def d_beside(q):
        return send(dys.at[blocks(q)], dyb.at[blocks(q)], y_send.at[q], y_recv.at[q], beside)

    def d_across(q):
        there = dec.at[tp, blocks(q)]
        return send(there, there, l_send.at[q, 0], l_recv.at[q, tp], across)

    def d_over_z(q, dz, other):
        mine = z * 2 + (1 - yh if other else yh)
        there = dec.at[mine, blocks(q)]
        return send(there, there, l_send.at[q, dz + 3 * other], l_recv.at[q, mine],
                    device(x, yl, c, (z + dz) % 4, yh))

    def d_multiply(q):
        start, width = SPANS[q]
        columns = slice(start * LANE, (start + width) * LANE)

        @pl.loop(0, 8)
        def _(n):
            xg, side = (x + n // 2 + 2) % 4, n % 2
            block = jnp.dot(aa[side * 8 + (1 - c) * 4 + xg], wb[:, columns], preferred_element_type=F32)
            for b in range(width):
                dgive[xg, side, start + b] = block[:, b * LANE : (b + 1) * LANE].astype(BF)

            @pl.when(side == 1)
            def _():
                d_hand(q, xg).start()

        @pl.loop(0, 8)
        def _(n):
            dx, side = (n // 2 + 2) % 4, n % 2
            xg = (x + dx) % 4
            block = jnp.dot(aa[side * 8 + c * 4 + xg], wb[:, columns], preferred_element_type=F32)

            @pl.when(side == 0)
            def _():
                d_hand(q, xg).wait_recv()

            for b in range(width):
                dpart[xg, side, start + b] = (
                    block[:, b * LANE : (b + 1) * LANE] + dgot[xg, side, start + b].astype(F32)
                ).astype(BF)

            if q == 0:
                @pl.when(jnp.logical_and(side == 1, dx != 0))
                def _():
                    d_over_x(q, dx).start()

    def d_x_sum(q):
        start, width = SPANS[q]
        for dx in (1, 3, 2):
            d_over_x(q, dx).wait_recv()

        def total(side, b):
            value = dpart[x, side, b].astype(F32)
            for slot in range(3):
                value = value + dxb[slot, side, b].astype(F32)
            return value

        for b in range(start, start + width):
            dys[b] = total(1 - yl, b).astype(BF)
        d_beside(q).start()
        for b in range(start, start + width):
            dkeep[b] = total(yl, b)

    def d_finish(q):
        start, width = SPANS[q]
        d_beside(q).wait_recv()
        for b in range(start, start + width):
            dec[tp, b] = (dkeep[b] + dyb[b].astype(F32)).astype(BF)
        for dz in (2, 1, 3):
            d_over_z(q, dz, 0).start()
        d_across(q).start()

    def d_pass(q):
        other = dec.at[z * 2 + 1 - yh, blocks(q)]
        pltpu.make_async_copy(other, other, l_recv.at[q, z * 2 + 1 - yh]).wait()
        for dz in (2, 1, 3):
            d_over_z(q, dz, 1).start()

    parts = len(SPANS)
    for q in range(parts):
        d_multiply(q)
    for q in range(parts + 1):
        if q < parts:
            d_x_sum(q)
        if q + 1 < parts:
            for dx in (2, 1, 3):
                d_over_x(q + 1, dx).start()
        if q > 0:
            d_pass(q - 1)
        if q < parts:
            d_finish(q)

    for q in range(len(SPANS)):
        start, width = SPANS[q]

        @pl.loop(2, 8)
        def _(d):
            t = (z * 2 + d) % 8
            pltpu.make_async_copy(dec.at[t, blocks(q)], dec.at[t, blocks(q)], l_recv.at[q, t]).wait()

        for t in range(8):
            for b in range(start, start + width):
                decoded[:, t * 640 + b * LANE : t * 640 + (b + 1) * LANE] = dec[t, b]

    for j in range(CHUNKS):
        for copy in (own_up(j), own_dn(j), fwd_up(j), fwd_dn(j)) + (trade(j),):
            copy.wait_send()

        @pl.loop(0, 4)
        def _(r):
          hand(j, r).wait_send()

        if j < len(SPANS):
          @pl.loop(0, 4)
          def _(k):
            d_hand(j, k).wait_send()

          d_beside(j).wait_send()
          d_across(j).wait_send()
          for dz in (1, 2, 3):
            d_over_x(j, dz).wait_send()
            d_over_z(j, dz, 0).wait_send()
            d_over_z(j, dz, 1).wait_send()

        for dx in (1, 2, 3):
            over_x(j, 0, dx).wait_send()
        for piece in pieces(j):
          @pl.when(jnp.logical_not(is_me(piece[2])))
          def _():
              to_owner(j, piece, False).wait_send()

    for dz in (1, 2, 3):
      heads_z(dz).wait_send()

    @pl.loop(0, 4)
    def _(dz):
      @pl.when(jnp.logical_not(stays_x(dz)))
      def _():
          heads_x(dz, False).wait_send()

    for h in range(2):
      for other in range(2):
          @pl.when(jnp.logical_not(stays(h, other)))
          def _():
              spread(h, other, False).wait_send()


def learn_and_decode(
    context, out_grad, rewards, lengths, cosine, sine, tokens_in, w_query, w_query_rows, w_key, w_value,
    old_keys, old_values, master, first_moment, second_moment,
):
    dma = pltpu.SemaphoreType.DMA
    vmem = pltpu.VMEM
    tokens, width = context.shape
    anywhere = pl.BlockSpec(memory_space=pl.ANY)
    in_smem = pl.BlockSpec(memory_space=pltpu.SMEM)
    in_vmem = pl.BlockSpec(memory_space=pltpu.VMEM)
    grid_all = [anywhere] * 2 + [in_smem] * 2 + [in_vmem] * 2 + [anywhere] * 10
    return pl.pallas_call(
        step_kernel,
        out_shape=(
            jax.ShapeDtypeStruct((ROWS, width), F32),
            jax.ShapeDtypeStruct((LANE, 8 * width), BF),
        ),
        in_specs=grid_all,
        out_specs=(pl.BlockSpec(memory_space=pltpu.VMEM), pl.BlockSpec(memory_space=pltpu.VMEM)),
        scratch_shapes=[
            vmem((4, CHUNKS, tokens, LANE), BF),
            vmem((2, CHUNKS, tokens, LANE), BF),
            vmem((2, tokens, width), BF),
            vmem((16, 8, LANE), F32),
            vmem((8, LANE), F32),
            vmem((12, LANE, width), F32),
            vmem((CHUNKS, 4, LANE, width), BF),
            vmem((CHUNKS, 4, LANE, width), BF),
            vmem((CHUNKS, 4, LANE, width), BF),
            vmem((CHUNKS, 3, LANE, width), BF),
            vmem((CHUNKS, LANE, width), BF),
            vmem((2, ROWS, width), BF),
            vmem((4, width, LANE), BF),
            vmem((4, width, LANE), BF),
            vmem((4, 4, ROWS, LANE), BF),
            vmem((16, LANE, ROWS), BF),
            vmem((ROWS, width), BF),
            vmem((4, 2, CHUNKS, LANE, LANE), BF),
            vmem((4, 2, CHUNKS, LANE, LANE), BF),
            vmem((4, 2, CHUNKS, LANE, LANE), BF),
            vmem((3, 2, CHUNKS, LANE, LANE), BF),
            vmem((CHUNKS, LANE, LANE), F32),
            vmem((CHUNKS, LANE, LANE), BF),
            vmem((CHUNKS, LANE, LANE), BF),
            vmem((8, CHUNKS, LANE, LANE), BF),
            dma((2, CHUNKS)),
            dma((2, CHUNKS)), dma((2, CHUNKS)),
            dma((2, CHUNKS)), dma((2, CHUNKS)),
            dma((CHUNKS,)), dma((CHUNKS,)),
            dma((16,)), dma((16,)),
            dma((CHUNKS, 4)), dma((CHUNKS, 4)),
            dma((CHUNKS, 3)), dma((CHUNKS, 3)),
            dma((CHUNKS, 2)), dma((2, 3)),
            dma((4,)), dma((4,)),
            dma((4,)), dma((4,)),
            dma((2, 2)), dma((4,)),
            dma((3, 4)), dma((3, 4)),
            dma((3, 3)), dma((3, 3)),
            dma((3,)), dma((3,)),
            dma((3, 7)), dma((3, 8)),
            vmem((LANE, 8 * width), BF),
            vmem((LANE, width), F32), vmem((LANE, LANE), F32), vmem((LANE, LANE), F32),
            vmem((32, 24, LANE), F32), vmem((32, 16, LANE), F32), vmem((32, 16, LANE), F32),
            vmem((4, 8, CACHE + 16, LANE), BF), vmem((4, 8, CACHE + 16, LANE), BF),
            vmem((32, 24, LANE), F32), vmem((LANE, LANE), F32),
            vmem((ROWS, width), F32), vmem((ROWS, width), F32), vmem((ROWS, width), F32),
            dma((5,)), dma((4, 2)), dma((4,)),
        ],
        compiler_params=pltpu.CompilerParams(
            collective_id=0, has_side_effects=True, vmem_limit_bytes=63 * 1024 * 1024
        ),
        cost_estimate=pl.CostEstimate(flops=14_300_000_000, bytes_accessed=10_000_000, transcendentals=0),
        name="learn_and_decode",
    )(
        context, out_grad, rewards, lengths, cosine, sine, tokens_in, w_query, w_query_rows, w_key, w_value,
        old_keys, old_values, master, first_moment, second_moment,
    )


def per_device(
    context,
    out_grad,
    rewards,
    master,
    first_moment,
    second_moment,
    inputs,
    w_query,
    w_key,
    w_value,
    cache_keys,
    cache_values,
    lengths,
):
    step_total, seq_local, model_width = inputs.shape
    seq_length = jnp.repeat(lengths, seq_local // lengths.shape[0])
    positions = seq_length[None, :] + jnp.arange(step_total, dtype=jnp.int32)[:, None]
    half_dim = HEAD_DIM // 2
    frequency = rope_base ** (-2.0 * jnp.arange(half_dim, dtype=F32) / HEAD_DIM)
    angles = positions.reshape(-1, 1).astype(F32) * frequency
    cosine = jnp.concatenate([jnp.cos(angles), jnp.cos(angles)], axis=1)
    sine = jnp.concatenate([-jnp.sin(angles), jnp.sin(angles)], axis=1)
    adam_step, decoded = learn_and_decode(
        context, out_grad, rewards, lengths, cosine, sine,
        inputs.reshape(step_total * seq_local, model_width),
        w_query.reshape(10, 4, LANE, 5 * LANE), w_query,
        w_key.reshape(4, 2, CHUNKS, LANE, LANE), w_value.reshape(4, 2, CHUNKS, LANE, LANE),
        cache_keys, cache_values, master, first_moment, second_moment,
    )
    return (decoded.reshape(step_total, seq_local, model_width), adam_step)


def solution(mesh):
    placed = (
        P("rep", "tp"),
        P("rep", "tp"),
        P(None, "rep"),
        P("rep", "tp"),
        P("rep", "tp"),
        P("rep", "tp"),
        P(None, "rep", None),
        P(None, "tp"),
        P(None, "tp"),
        P(None, "tp"),
        P("rep", None, "tp"),
        P("rep", None, "tp"),
        P("rep"),
    )
    return jax.shard_map(
        per_device,
        mesh=mesh,
        in_specs=placed,
        out_specs=(P(None, "rep", None), P("rep", "tp")),
        check_vma=False,
    )
```
